16 devices in a mesh: dp: 2 (over y, z), ep: 8 (over x, core).
Axes of the slice: x: 4, y: 2, z: 1, core: 2. Of those that a mesh axis runs over, the one named last changes fastest.
The devices are a block of a 4x4x8 slice.
Arguments:
- x_in: bfloat16 [1536, 2048], P(('dp', 'ep')), parts along dimension 0
- norm_gain: bfloat16 [2048], replicated
- w_router: bfloat16 [2048, 64], replicated
- expert_ids: int32 [1536, 8], P(('dp', 'ep')), parts along dimension 0
- w_gate: bfloat16 [64, 2048, 1024], P('ep')
- w_up: bfloat16 [64, 2048, 1024], P('ep')
- w_down: bfloat16 [64, 1024, 2048], P('ep')
Outputs:
- output: bfloat16 [1536, 2048], P(('dp', 'ep')), parts along dimension 0
There are 2 independent parts. The reference program is written for one: setup_inputs(seed, part) draws one part's arguments, and reference() takes and returns one part's arrays. A program takes and returns all parts, laid end to end along the dimension named above; an argument that names none is the same for every part.
All inputs are finite; a program needn't handle non-finite values.
Results may differ from the reference program's by a relative error of at most 0.00121.
Values are sent between devices in bfloat16 or wider.
A program may use at most 768 MiB of HBM per device.

```python
import jax
import jax.numpy as jnp
from jax import lax

HIDDEN = 2048
EXPERT_FF = 1024
EXPERTS = 64
TOP_K = 8
TOKENS = 96
GROUP_SIZE = 8

EPS = 1e-6
CAP_DEV = 2 * TOKENS * TOP_K // EXPERTS
HOT_COUNT = EXPERTS // 4
COLD_LEFT = TOKENS * TOP_K - HOT_COUNT * CAP_DEV
COLD_BASE = COLD_LEFT // (EXPERTS - HOT_COUNT)
COLD_EXTRA = COLD_LEFT % (EXPERTS - HOT_COUNT)
ROW_LIMIT = GROUP_SIZE * CAP_DEV


def draw_device(hot_flag, key):
    key_rank, key_rows, key_cols = jax.random.split(key, 3)
    expert_range = jnp.arange(EXPERTS, dtype=jnp.int32)
    noise = jax.random.randint(key_rank, (EXPERTS,), 0, EXPERTS, dtype=jnp.int32)
    score = (1 - hot_flag) * (EXPERTS * EXPERTS) + noise * EXPERTS + expert_range
    rank = jnp.argsort(jnp.argsort(score))
    counts = jnp.where(rank < HOT_COUNT, CAP_DEV, COLD_BASE + (rank - HOT_COUNT < COLD_EXTRA).astype(jnp.int32))
    bounds = jnp.cumsum(counts).astype(jnp.int32)
    flat_ids = jnp.searchsorted(bounds, jnp.arange(TOKENS * TOP_K, dtype=jnp.int32), side="right").astype(jnp.int32)
    table = flat_ids.reshape(TOP_K, TOKENS).T
    table = jax.random.permutation(key_rows, table, axis=0)
    col_score = jax.random.randint(key_cols, (TOKENS, TOP_K), 0, TOP_K, dtype=jnp.int32) * TOP_K + jnp.arange(TOP_K, dtype=jnp.int32)
    col_order = jnp.argsort(col_score, axis=1)
    return jnp.take_along_axis(table, col_order, axis=1)


def draw_routes(key):
    key_hot, key_dev = jax.random.split(key)
    hot_order = jax.random.permutation(key_hot, EXPERTS)
    hot_flag = (jnp.argsort(hot_order) < HOT_COUNT).astype(jnp.int32)
    dev_keys = jax.random.split(key_dev, GROUP_SIZE)
    routes = jax.vmap(draw_device, in_axes=(None, 0))(hot_flag, dev_keys)
    return routes.reshape(GROUP_SIZE * TOKENS, TOP_K).astype(jnp.int32)


def setup_inputs(seed: int = 0, part: int = 0) -> dict:
    shared = jax.random.split(jax.random.key(seed), 5)
    own = jax.random.split(jax.random.fold_in(jax.random.key(seed + 1), part), 2)
    x_in = (0.5 * jax.random.normal(own[0], (GROUP_SIZE * TOKENS, HIDDEN), jnp.float32)).astype(jnp.bfloat16)
    norm_gain = jax.random.uniform(shared[0], (HIDDEN,), jnp.float32, 0.5, 1.5).astype(jnp.bfloat16)
    w_router = (2.0 * HIDDEN ** -0.5 * jax.random.normal(shared[1], (HIDDEN, EXPERTS), jnp.float32)).astype(jnp.bfloat16)
    w_gate = (HIDDEN ** -0.5 * jax.random.normal(shared[2], (EXPERTS, HIDDEN, EXPERT_FF), jnp.float32)).astype(jnp.bfloat16)
    w_up = (HIDDEN ** -0.5 * jax.random.normal(shared[3], (EXPERTS, HIDDEN, EXPERT_FF), jnp.float32)).astype(jnp.bfloat16)
    w_down = (1.5 * EXPERT_FF ** -0.5 * jax.random.normal(shared[4], (EXPERTS, EXPERT_FF, HIDDEN), jnp.float32)).astype(jnp.bfloat16)
    expert_ids = draw_routes(own[1])
    return {"x_in": x_in, "norm_gain": norm_gain, "w_router": w_router, "expert_ids": expert_ids, "w_gate": w_gate, "w_up": w_up, "w_down": w_down}


def reference(x_in, norm_gain, w_router, expert_ids, w_gate, w_up, w_down):
    resid = x_in.astype(jnp.float32)
    mean_sq = jnp.mean(resid * resid, axis=-1, keepdims=True)
    normed = (resid * lax.rsqrt(mean_sq + EPS) * norm_gain.astype(jnp.float32)).astype(jnp.bfloat16)
    logits = jnp.dot(normed, w_router, preferred_element_type=jnp.float32)
    router_p = jax.nn.softmax(logits, axis=-1)
    picked = jnp.take_along_axis(router_p, expert_ids, axis=1)
    gates = picked / jnp.sum(picked, axis=1, keepdims=True)
    total = x_in.shape[0]

    def one_expert(moe_sum, inputs):
        expert, gate_w, up_w, down_w = inputs
        hits = expert_ids == expert
        weight = jnp.sum(jnp.where(hits, gates, 0.0), axis=1)
        rows = jnp.nonzero(jnp.any(hits, axis=1), size=ROW_LIMIT, fill_value=total)[0]
        sel_rows = jnp.take(normed, rows, axis=0, mode="fill", fill_value=0)
        gate_val = jnp.dot(sel_rows, gate_w, preferred_element_type=jnp.float32)
        up_val = jnp.dot(sel_rows, up_w, preferred_element_type=jnp.float32)
        hidden_act = (jax.nn.silu(gate_val) * up_val).astype(jnp.bfloat16)
        out_rows = jnp.dot(hidden_act, down_w, preferred_element_type=jnp.float32).astype(jnp.bfloat16)
        row_w = jnp.take(weight, rows, mode="fill", fill_value=0)
        moe_sum = moe_sum.at[rows].add(out_rows.astype(jnp.float32) * row_w[:, None], mode="drop")
        return moe_sum, None

    start_sum = jnp.zeros((total, HIDDEN), jnp.float32)
    moe_sum = lax.scan(one_expert, start_sum, (jnp.arange(EXPERTS, dtype=jnp.int32), w_gate, w_up, w_down))[0]
    return (resid + moe_sum).astype(jnp.bfloat16)
```

```python
import functools

import jax
import jax.numpy as jnp
from jax import lax
from jax.experimental import pallas as pl
from jax.experimental.pallas import tpu as pltpu
from jax.sharding import PartitionSpec as P

EPS = 1e-6
F32 = jnp.float32
BF16 = jnp.bfloat16
COLS = 256
LANES = 128
RING = 8


def dot(a, b):
    return jnp.dot(a, b, preferred_element_type=F32)


def moe_kernel(
    x_ref, gain_ref, wr_ref, ids_ref, wg_ref, wu_ref, wd_ref, out_ref,
    wbuf, xbuf, hbuf, xe, act, oh, gates, a3, ybuf, ps, d2d, far, fin, lg, ids_all, soft, mask,
    wsem, ids_s, ids_r, ag_s, ag_r, d2d_s, d2d_r, far_s, far_r, fin_s, fin_r,
):
    tokens, hidden = x_ref.shape
    local_experts = act.shape[0]
    experts = wr_ref.shape[1]
    chips = xbuf.shape[0]
    half = tokens // 2
    pair_cap = oh.shape[0] // local_experts
    cap = pair_cap // 2
    chunks = hidden // COLS

    me = lax.axis_index("ep")
    chip, core = me // 2, lax.rem(me, 2)

    def device(r, q):
        return {"ep": lax.rem(chip + r, chips) * 2 + (lax.rem(core + q, 2))}

    right, left, peer = device(1, 0), device(chips - 1, 0), device(0, 1)

    def remote(src, dst, send, recv, to):
        return pltpu.make_async_remote_copy(
            src_ref=src, dst_ref=dst, send_sem=send, recv_sem=recv,
            device_id=to, device_id_type=pl.DeviceIdType.MESH,
        )

    def start_gate_up(e):
        slot = 2 * lax.rem(e, RING // 2)
        for k, w in enumerate((wg_ref, wu_ref)):
            for n in range(4):
                pltpu.make_async_copy(
                    w.at[e, :, :, pl.ds(n * COLS, COLS)], wbuf.at[slot + k, pl.ds(2 * n, 2)], wsem.at[slot + k]
                ).start()

    def start_down(n):
        for m in range(4):
            pltpu.make_async_copy(
                wd_ref.at[pl.ds(2 * m, 2), :, pl.ds(pl.multiple_of(n * COLS, COLS), COLS)],
                wbuf.at[n, pl.ds(2 * m, 2)], wsem.at[n]
            ).start()

    def wait_slot(slot):
        pltpu.make_async_copy(wbuf.at[slot], wbuf.at[slot], wsem.at[slot]).wait()

    for e in range(RING // 2):
        start_gate_up(e)

    soft[...] = jnp.full(soft.shape, -1.0, F32)
    soft[pl.ds(0, tokens), pl.ds(0, ids_ref.shape[1])] = ids_ref[...].astype(F32)
    ids_all[0, 0] = soft[:, 0:LANES].T[0:8, :]

    barrier = pltpu.get_barrier_semaphore()
    others = [(r, q) for r in range(chips) for q in range(2) if (r, q) != (0, 0)]
    for r, q in others:
        pl.semaphore_signal(barrier, inc=1, device_id=device(r, q), device_id_type=pl.DeviceIdType.MESH)
    pl.semaphore_wait(barrier, len(others))

    top, bot = pl.ds(0, half), pl.ds(half, half)
    last = chips - 1
    c_r0 = remote(x_ref.at[top], xbuf.at[last, 0, top], ag_s.at[0], ag_r.at[last, 0, 0], right)
    c_l1 = remote(x_ref.at[bot], xbuf.at[1, 0, bot], ag_s.at[1], ag_r.at[1, 0, 1], left)
    c_r1 = remote(x_ref.at[bot], xbuf.at[last, 0, bot], ag_s.at[2], ag_r.at[last, 0, 1], right)
    c_l0 = remote(x_ref.at[top], xbuf.at[1, 0, top], ag_s.at[3], ag_r.at[1, 0, 0], left)
    c_p = remote(x_ref, xbuf.at[0, 1], ag_s.at[4], ag_r.at[0, 1, 0], peer)
    ids_c = {}
    for r, q in others:
        back = (chips - r) % chips
        ids_c[(back, q)] = remote(
            ids_all.at[0, 0], ids_all.at[back, q], ids_s.at[r, q], ids_r.at[back, q], device(r, q)
        )
    ids_c[(0, 1)].start()
    c_p.start()
    for k in others:
        if k != (0, 1):
            ids_c[k].start()
    for c in (c_r0, c_l1, c_r1, c_l0):
        c.start()
    f_r = remote(xbuf.at[last, 0, top], xbuf.at[2, 0, top], ag_s.at[5], ag_r.at[2, 0, 0], right)
    f_l = remote(xbuf.at[1, 0, bot], xbuf.at[2, 0, bot], ag_s.at[6], ag_r.at[2, 0, 1], left)
    cross = {}
    for k, r in enumerate((last, 1, 2)):
        for h, rows in enumerate((top, bot)):
            cross[(r, h)] = remote(
                xbuf.at[r, 0, rows], xbuf.at[r, 1, rows], ag_s.at[7 + 2 * k + h], ag_r.at[r, 1, h], peer
            )

    hbuf[...] = jnp.zeros_like(hbuf)
    gain = gain_ref[...].astype(F32)
    tri = (
        lax.broadcasted_iota(jnp.int32, (LANES, LANES), 0) < lax.broadcasted_iota(jnp.int32, (LANES, LANES), 1)
    ).astype(BF16)

    def process(r, sources):
        for q, src in enumerate(sources):
            def norm_rows(g, carry, q=q, src=src):
                rows = pl.ds(pl.multiple_of(g * 16, 16), 16)
                v = src[rows, :].astype(F32)
                ms = jnp.mean(v * v, axis=-1, keepdims=True)
                hv = (v * lax.rsqrt(ms + EPS) * gain).astype(BF16)
                hbuf[pl.ds(pl.multiple_of(q * LANES + g * 16, 16), 16), :] = hv
                return carry
            lax.fori_loop(0, tokens // 16, norm_rows, 0)
        lg[:, 0:experts] = dot(hbuf[...], wr_ref[...])
        logits = lg[...].T[0:experts, :]
        shifted = jnp.exp(logits - jnp.max(logits, axis=0, keepdims=True))
        prob = shifted / jnp.sum(shifted, axis=0, keepdims=True)
        ids = jnp.concatenate([ids_all[r, 0], ids_all[r, 1]], axis=1)
        eid = lax.broadcasted_iota(jnp.int32, prob.shape, 0).astype(F32)
        chosen = eid == ids[0:1, :]
        for j in range(1, ids.shape[0]):
            chosen = chosen | (eid == ids[j : j + 1, :])
        picked = jnp.where(chosen, prob, 0.0)
        gate_all = jnp.where(chosen, picked / jnp.sum(picked, axis=0, keepdims=True), 0.0)
        soft[0:experts, :] = gate_all
        mask[...] = jnp.where(chosen, 1.0, 0.0)
        mine = pl.ds(pl.multiple_of(me * local_experts, local_experts), local_experts)
        gate = soft[mine, :]
        hit = mask[mine, :]
        pos = jnp.concatenate(
            [dot(hit[:, q * LANES : (q + 1) * LANES].astype(BF16), tri) + float(q * cap) for q in range(2)], axis=1
        )
        pos = jnp.where(hit > 0.5, pos, -1.0)
        slot = lax.broadcasted_iota(jnp.int32, (pair_cap, 2 * LANES), 0).astype(F32)
        for e in range(local_experts):
            here = slot == pos[e : e + 1, :]
            oh[pl.ds(e * pair_cap, pair_cap), :] = jnp.where(here, 1.0, 0.0).astype(BF16)
            gates[pl.ds(e * pair_cap, pair_cap), :] = jnp.where(here, gate[e : e + 1, :], 0.0)

        def gather_cols(n, carry):
            cols = pl.ds(pl.multiple_of(n * COLS, COLS), COLS)
            res = dot(oh[...], hbuf[:, cols]).astype(BF16)
            for e in range(local_experts):
                xe[e, pl.ds(r * pair_cap, pair_cap), cols] = res[e * pair_cap : (e + 1) * pair_cap]
            return carry
        lax.fori_loop(0, hidden // COLS, gather_cols, 0)

        gt = gates[...].T
        hi = gt.astype(BF16)
        rest = gt - hi.astype(F32)
        mid = rest.astype(BF16)
        low = (rest - mid.astype(F32)).astype(BF16)
        for k, part in enumerate((hi, mid, low)):
            for q in range(2):
                a3[r, pl.ds((2 * k + q) * tokens, tokens), :] = part[q * LANES : q * LANES + tokens]

    def ids_wait(r):
        for q in range(2):
            if (r, q) != (0, 0):
                ids_c[(r, q)].wait_recv()

    ids_wait(0)
    c_p.wait_recv()
    process(0, (x_ref, xbuf.at[0, 1]))
    c_r0.wait_recv()
    f_r.start()
    cross[(last, 0)].start()
    c_l1.wait_recv()
    f_l.start()
    cross[(1, 1)].start()
    c_r1.wait_recv()
    cross[(last, 1)].start()
    c_l0.wait_recv()
    cross[(1, 0)].start()
    for r in (last, 1):
        ids_wait(r)
        cross[(r, 0)].wait_recv()
        cross[(r, 1)].wait_recv()
        process(r, (xbuf.at[r, 0], xbuf.at[r, 1]))
    f_r.wait_recv()
    cross[(2, 0)].start()
    f_l.wait_recv()
    cross[(2, 1)].start()
    ids_wait(2)
    cross[(2, 0)].wait_recv()
    cross[(2, 1)].wait_recv()
    process(2, (xbuf.at[2, 0], xbuf.at[2, 1]))

    def expert(e, carry):
        slot = 2 * lax.rem(e, RING // 2)
        wait_slot(slot)
        wait_slot(slot + 1)
        rows = xe[e]
        for n in range(4):
            g = dot(rows, wbuf[slot, 2 * n : 2 * n + 2].reshape(hidden, COLS))
            u = dot(rows, wbuf[slot + 1, 2 * n : 2 * n + 2].reshape(hidden, COLS))
            act[e, :, n * COLS : (n + 1) * COLS] = (g * jax.nn.sigmoid(g) * u).astype(BF16)

        @pl.when(e < local_experts - RING // 2)
        def _():
            start_gate_up(e + RING // 2)

        @pl.when(e >= local_experts - RING // 2)
        def _():
            n = 2 * (e - (local_experts - RING // 2))
            start_down(n)
            start_down(n + 1)
        return carry

    lax.fori_loop(0, local_experts, expert, 0)

    def cross_copy(n):
        return remote(ps.at[n, 1], d2d.at[n], d2d_s.at[n], d2d_r.at[n], peer)

    def far_copies(n):
        return (
            remote(ps.at[n, 0, 2, 0], far.at[n, 0], far_s.at[n, 0], far_r.at[n, 0], right),
            remote(ps.at[n, 0, 2, 1], far.at[n, 1], far_s.at[n, 1], far_r.at[n, 1], left),
        )

    def near_copies(n):
        return (
            remote(ps.at[n, 0, 1, 1], fin.at[n, 0, 1], fin_s.at[n, 0, 1], fin_r.at[n, 0, 1], right),
            remote(ps.at[n, 0, last, 0], fin.at[n, 1, 0], fin_s.at[n, 1, 0], fin_r.at[n, 1, 0], left),
        )

    def sum_copies(n):
        return (
            remote(ps.at[n, 0, 1, 0], fin.at[n, 0, 0], fin_s.at[n, 0, 0], fin_r.at[n, 0, 0], right),
            remote(ps.at[n, 0, last, 1], fin.at[n, 1, 1], fin_s.at[n, 1, 1], fin_r.at[n, 1, 1], left),
        )

    def stage1(n):
        cross_copy(n).wait_recv()
        for r in (2, 1, last, 0):
            ps[n, 0, r] = ps[n, 0, r] + d2d[n, r]
        for c in far_copies(n) + near_copies(n):
            c.start()

    def chunk(n, carry):
        wait_slot(n)
        for e in range(local_experts):
            y = dot(act[e], wbuf[n, e]).astype(BF16)
            for r in range(chips):
                ybuf[r, pl.ds(e * pair_cap, pair_cap), :] = y[r * pair_cap : (r + 1) * pair_cap]
        for r in range(chips):
            parts = dot(a3[r], ybuf[r])
            t = 2 * tokens
            total = parts[0:t] + (parts[t : 2 * t] + parts[2 * t : 3 * t])
            for q in range(2):
                for h in range(2):
                    ps[n, q, r, h] = total[q * tokens : (q + 1) * tokens, h * LANES : (h + 1) * LANES]
        cross_copy(n).start()

        @pl.when(n > 0)
        def _():
            stage1(n - 1)
        return carry

    lax.fori_loop(0, chunks, chunk, 0)
    stage1(chunks - 1)

    def stage2(n, carry):
        from_left, from_right = far_copies(n)
        to_right, to_left = sum_copies(n)
        from_left.wait_recv()
        ps[n, 0, 1, 0] = ps[n, 0, 1, 0] + far[n, 0]
        to_right.start()
        from_right.wait_recv()
        ps[n, 0, last, 1] = ps[n, 0, last, 1] + far[n, 1]
        to_left.start()
        return carry

    lax.fori_loop(0, chunks, stage2, 0)

    def final(n, carry):
        for c in near_copies(n) + sum_copies(n):
            c.wait_recv()
        for h in range(2):
            cols = pl.ds(pl.multiple_of(n * COLS + h * LANES, LANES), LANES)
            total = ps[n, 0, 0, h] + fin[n, 0, h] + fin[n, 1, h]
            out_ref[:, cols] = (x_ref[:, cols].astype(F32) + total).astype(BF16)
        return carry

    lax.fori_loop(0, chunks, final, 0)

    def drain(n, carry):
        cross_copy(n).wait_send()
        for c in far_copies(n) + near_copies(n) + sum_copies(n):
            c.wait_send()
        return carry

    lax.fori_loop(0, chunks, drain, 0)
    for c in [c_r0, c_l1, c_r1, c_l0, c_p, f_r, f_l] + list(ids_c.values()) + list(cross.values()):
        c.wait_send()


def solution(mesh):
    group = mesh.shape["ep"]
    chips = group // 2

    def local_block(x_in, norm_gain, w_router, expert_ids, w_gate, w_up, w_down):
        tokens, hidden = x_in.shape
        experts = w_router.shape[1]
        top_k = expert_ids.shape[1]
        local_experts, _, ff = w_gate.shape
        cap = 2 * tokens * top_k // experts
        rows = local_experts * 2 * cap
        chunks = hidden // COLS
        wg = w_gate.reshape(local_experts, 2, hidden // 2, ff)
        wu = w_up.reshape(local_experts, 2, hidden // 2, ff)
        vmem = pl.BlockSpec(memory_space=pltpu.VMEM)
        hbm = pl.BlockSpec(memory_space=pl.ANY)
        dma = pltpu.SemaphoreType.DMA
        return pl.pallas_call(
            moe_kernel,
            out_shape=jax.ShapeDtypeStruct((tokens, hidden), BF16),
            in_specs=[vmem, vmem, vmem, vmem, hbm, hbm, hbm],
            out_specs=vmem,
            scratch_shapes=[
                pltpu.VMEM((RING, local_experts, ff, COLS), BF16),
                pltpu.VMEM((chips, 2, tokens, hidden), BF16),
                pltpu.VMEM((2 * LANES, hidden), BF16),
                pltpu.VMEM((local_experts, group * cap, hidden), BF16),
                pltpu.VMEM((local_experts, group * cap, ff), BF16),
                pltpu.VMEM((rows, 2 * LANES), BF16),
                pltpu.VMEM((rows, 2 * LANES), F32),
                pltpu.VMEM((chips, 6 * tokens, rows), BF16),
                pltpu.VMEM((chips, rows, COLS), BF16),
                pltpu.VMEM((chunks, 2, chips, 2, tokens, LANES), F32),
                pltpu.VMEM((chunks, chips, 2, tokens, LANES), F32),
                pltpu.VMEM((chunks, 2, tokens, LANES), F32),
                pltpu.VMEM((chunks, 2, 2, tokens, LANES), F32),
                pltpu.VMEM((2 * LANES, LANES), F32),
                pltpu.VMEM((chips, 2, 8, LANES), F32),
                pltpu.VMEM((LANES, 2 * LANES), F32),
                pltpu.VMEM((experts, 2 * LANES), F32),
                dma((RING,)),
                dma((chips, 2)), dma((chips, 2)),
                dma((13,)), dma((chips, 2, 2)),
                dma((chunks,)), dma((chunks,)),
                dma((chunks, 2)), dma((chunks, 2)),
                dma((chunks, 2, 2)), dma((chunks, 2, 2)),
            ],
            compiler_params=pltpu.CompilerParams(
                collective_id=0, has_side_effects=True, vmem_limit_bytes=67043328
            ),
        )(x_in, norm_gain.reshape(1, hidden), w_router, expert_ids, wg, wu, w_down)

    tok_spec = P(("dp", "ep"), None)
    expert_spec = P("ep", None, None)
    return jax.shard_map(local_block, mesh=mesh, in_specs=(tok_spec, P(None), P(None, None), tok_spec, expert_spec, expert_spec, expert_spec), out_specs=tok_spec, check_vma=False)
```

```python
import functools

import jax
import jax.numpy as jnp
from jax import lax
from jax.experimental import pallas as pl
from jax.experimental.pallas import tpu as pltpu
from jax.sharding import PartitionSpec as P

EPS = 1e-6
F32 = jnp.float32
BF16 = jnp.bfloat16
COLS = 256
LANES = 128
RING = 8


def dot(a, b):
    return jnp.dot(a, b, preferred_element_type=F32)


def moe_kernel(
    x_hbm, gain_hbm, wr_hbm, ids_hbm, wg_ref, wu_ref, wd_ref, out_ref,
    x_ref, gain_ref, wr_ref, ids_ref,
    wbuf, xbuf, hbuf, xe, act, oh, gates, a3, ybuf, ps, d2d, far, fin, ids_all, soft, mask,
    in_sem, wsem, ids_s, ids_r, ag_s, ag_r, d2d_s, d2d_r, far_s, far_r, fin_s, fin_r,
):
    tokens, hidden = x_ref.shape
    local_experts = act.shape[0]
    experts = wr_ref.shape[0]
    chips = xbuf.shape[0]
    half = tokens // 2
    pair_cap = oh.shape[0] // local_experts
    own_cap = 2 * pair_cap // 3
    chunks = hidden // COLS

    me = lax.axis_index("ep")
    chip, core = me // 2, lax.rem(me, 2)

    def device(r, q):
        return {"ep": lax.rem(chip + r, chips) * 2 + (lax.rem(core + q, 2))}

    right, left, peer = device(1, 0), device(chips - 1, 0), device(0, 1)

    def remote(src, dst, send, recv, to):
        return pltpu.make_async_remote_copy(
            src_ref=src, dst_ref=dst, send_sem=send, recv_sem=recv,
            device_id=to, device_id_type=pl.DeviceIdType.MESH,
        )

    def start_gate_up(e):
        slot = 2 * lax.rem(e, RING // 2)
        for k, w in enumerate((wg_ref, wu_ref)):
            for n in range(4):
                pltpu.make_async_copy(
                    w.at[e, :, :, pl.ds(n * COLS, COLS)], wbuf.at[slot + k, pl.ds(2 * n, 2)], wsem.at[slot + k]
                ).start()

    def start_down(n):
        for m in range(4):
            pltpu.make_async_copy(
                wd_ref.at[pl.ds(2 * m, 2), :, pl.ds(pl.multiple_of(n * COLS, COLS), COLS)],
                wbuf.at[n, pl.ds(2 * m, 2)], wsem.at[n]
            ).start()

    def wait_slot(slot):
        pltpu.make_async_copy(wbuf.at[slot], wbuf.at[slot], wsem.at[slot]).wait()

    barrier = pltpu.get_barrier_semaphore()
    others = [(r, q) for r in range(chips) for q in range(2) if (r, q) != (0, 0)]
    for r, q in others:
        pl.semaphore_signal(barrier, inc=1, device_id=device(r, q), device_id_type=pl.DeviceIdType.MESH)
    inputs = [
        pltpu.make_async_copy(a, b, in_sem.at[k])
        for k, (a, b) in enumerate(((ids_hbm, ids_ref), (x_hbm, x_ref), (gain_hbm, gain_ref), (wr_hbm, wr_ref)))
    ]
    for c in inputs:
        c.start()

    ids_all[0, 0] = jnp.full(ids_all.shape[2:], -1.0, F32)
    with jax.named_scope("inputs"):
        for c in inputs:
            c.wait()
    ids_all[0, 0, :, 0:tokens] = ids_ref[...].astype(F32)
    for e in range(RING // 2):
        start_gate_up(e)
    with jax.named_scope("barrier"):
        pl.semaphore_wait(barrier, len(others))

    top, bot = pl.ds(0, half), pl.ds(half, half)
    last = chips - 1
    c_r0 = remote(x_ref.at[top], xbuf.at[last, 0, top], ag_s.at[0], ag_r.at[last, 0, 0], right)
    c_l1 = remote(x_ref.at[bot], xbuf.at[1, 0, bot], ag_s.at[1], ag_r.at[1, 0, 1], left)
    c_r1 = remote(x_ref.at[bot], xbuf.at[last, 0, bot], ag_s.at[2], ag_r.at[last, 0, 1], right)
    c_l0 = remote(x_ref.at[top], xbuf.at[1, 0, top], ag_s.at[3], ag_r.at[1, 0, 0], left)
    c_p = remote(x_ref, xbuf.at[0, 1], ag_s.at[4], ag_r.at[0, 1, 0], peer)
    ids_c = {}
    for r, q in others:
        back = (chips - r) % chips
        ids_c[(back, q)] = remote(
            ids_all.at[0, 0], ids_all.at[back, q], ids_s.at[r, q], ids_r.at[back, q], device(r, q)
        )
    ids_c[(0, 1)].start()
    c_p.start()
    for k in others:
        if k != (0, 1):
            ids_c[k].start()
    for c in (c_r0, c_l1, c_r1, c_l0):
        c.start()
    f_r = remote(xbuf.at[last, 0, top], xbuf.at[2, 0, top], ag_s.at[5], ag_r.at[2, 0, 0], right)
    f_l = remote(xbuf.at[1, 0, bot], xbuf.at[2, 0, bot], ag_s.at[6], ag_r.at[2, 0, 1], left)
    cross = {}
    for k, r in enumerate((last, 1, 2)):
        for h, rows in enumerate((top, bot)):
            cross[(r, h)] = remote(
                xbuf.at[r, 0, rows], xbuf.at[r, 1, rows], ag_s.at[7 + 2 * k + h], ag_r.at[r, 1, h], peer
            )

    for k in range(hbuf.shape[0]):
        for q in range(2):
            hbuf[k, q * LANES + tokens : (q + 1) * LANES, :] = jnp.zeros((LANES - tokens, hidden), BF16)
    gain = jnp.concatenate([gain_ref[k : k + 1, :] for k in range(gain_ref.shape[0])], axis=1).astype(F32)
    tri = (
        lax.broadcasted_iota(jnp.int32, (LANES, LANES), 0) < lax.broadcasted_iota(jnp.int32, (LANES, LANES), 1)
    ).astype(BF16)

    def norm(src, k, q, h):
        for g in range(half // 16):
            row = h * half + g * 16
            v = src[row : row + 16, :].astype(F32)
            ms = jnp.mean(v * v, axis=-1, keepdims=True)
            hbuf[k, q * LANES + row : q * LANES + row + 16, :] = (v * lax.rsqrt(ms + EPS) * gain).astype(BF16)

    def route(r, k):
        logits = lax.dot_general(
            wr_ref[...], hbuf[k], (((1,), (1,)), ((), ())), preferred_element_type=F32
        )
        shifted = jnp.exp(logits - jnp.max(logits, axis=0, keepdims=True))
        prob = shifted / jnp.sum(shifted, axis=0, keepdims=True)
        ids = jnp.concatenate([ids_all[r, 0], ids_all[r, 1]], axis=1)
        eid = lax.broadcasted_iota(jnp.int32, prob.shape, 0).astype(F32)
        chosen = eid == ids[0:1, :]
        for j in range(1, ids.shape[0]):
            chosen = chosen | (eid == ids[j : j + 1, :])
        picked = jnp.where(chosen, prob, 0.0)
        soft[...] = jnp.where(chosen, picked / jnp.sum(picked, axis=0, keepdims=True), 0.0)
        mask[...] = jnp.where(chosen, 1.0, 0.0)
        mine = pl.ds(pl.multiple_of(me * local_experts, local_experts), local_experts)
        gate = soft[mine, :]
        hit = mask[mine, :]
        rows = []
        for q in range(2):
            lanes = slice(q * LANES, (q + 1) * LANES)
            pos = dot(hit[:, lanes].astype(BF16), tri)
            first = pos < 15.5
            own = jnp.where(hit[:, lanes] > 0.5, jnp.where(first, pos, pos + 8.0 * q), -1.0)
            rows.append(jnp.where(hit[:, lanes] > 0.5, jnp.where(first, pos + 16.0 * q, pos + (16.0 + 8.0 * q)), -1.0))
            slot = lax.broadcasted_iota(jnp.int32, (own_cap, LANES), 0).astype(F32)
            for e in range(local_experts):
                gates[r, q, pl.ds(e * own_cap, own_cap), :] = jnp.where(
                    slot == own[e : e + 1, :], gate[e : e + 1, lanes], 0.0
                )
        pair = jnp.concatenate(rows, axis=1)
        slot = lax.broadcasted_iota(jnp.int32, (pair_cap, 2 * LANES), 0).astype(F32)
        for e in range(local_experts):
            oh[pl.ds(e * pair_cap, pair_cap), :] = jnp.where(slot == pair[e : e + 1, :], 1.0, 0.0).astype(BF16)

    def gather(r, k):
        def gather_cols(n, carry):
            for m in range(4):
                cols = pl.ds(pl.multiple_of(n * (4 * COLS) + m * COLS, COLS), COLS)
                res = dot(oh[...], hbuf[k, :, cols]).astype(BF16)
                for e in range(local_experts):
                    xe[e, pl.ds(r * pair_cap, pair_cap), cols] = res[e * pair_cap : (e + 1) * pair_cap]
            return carry
        lax.fori_loop(0, hidden // (4 * COLS), gather_cols, 0)

    def split_gates(r):
        for q in range(2):
            gt = gates[r, q].T[0:tokens]
            hi = gt.astype(BF16)
            rest = gt - hi.astype(F32)
            mid = rest.astype(BF16)
            low = (rest - mid.astype(F32)).astype(BF16)
            for p, part in enumerate((hi, mid, low)):
                a3[r, q, pl.ds(p * tokens, tokens), :] = part

    def tables(r, k):
        with jax.named_scope(f"route#r={r}"):
            route(r, k)
        with jax.named_scope(f"gather#r={r}"):
            gather(r, k)

    def ids_wait(r):
        for q in range(2):
            if (r, q) != (0, 0):
                ids_c[(r, q)].wait_recv()

    def gate_up_rows(e, rows):
        slot = 2 * lax.rem(e, RING // 2)
        data = xe[e, rows, :]
        for n in range(4):
            g = dot(data, wbuf[slot, 2 * n : 2 * n + 2].reshape(hidden, COLS))
            u = dot(data, wbuf[slot + 1, 2 * n : 2 * n + 2].reshape(hidden, COLS))
            act[e, rows, n * COLS : (n + 1) * COLS] = (g * jax.nn.sigmoid(g) * u).astype(BF16)

    own_rows = pl.ds(0, pair_cap)
    rest_rows = pl.ds(pair_cap, (chips - 1) * pair_cap)
    all_rows = pl.ds(0, chips * pair_cap)

    def own_pass(e, carry):
        with jax.named_scope("own_pass"):
            wait_slot(2 * e)
            wait_slot(2 * e + 1)
            gate_up_rows(e, own_rows)
        return carry

    with jax.named_scope("norm_own"):
        norm(x_ref, 0, 0, 0)
        norm(x_ref, 0, 0, 1)
    with jax.named_scope("own_wait"):
        ids_wait(0)
        c_p.wait_recv()
    with jax.named_scope("norm_peer"):
        norm(xbuf.at[0, 1], 0, 1, 0)
        norm(xbuf.at[0, 1], 0, 1, 1)
    tables(0, 0)
    lax.fori_loop(0, 2, own_pass, 0)
    with jax.named_scope("near_wait"):
        c_r0.wait_recv()
        f_r.start()
        cross[(last, 0)].start()
        c_l1.wait_recv()
        f_l.start()
        cross[(1, 1)].start()
    with jax.named_scope("norm_near"):
        norm(xbuf.at[last, 0], 0, 0, 0)
        norm(xbuf.at[1, 0], 1, 0, 1)
        cross[(last, 0)].wait_recv()
        cross[(1, 1)].wait_recv()
        norm(xbuf.at[last, 1], 0, 1, 0)
        norm(xbuf.at[1, 1], 1, 1, 1)
    lax.fori_loop(2, RING // 2, own_pass, 0)
    with jax.named_scope("near_wait2"):
        c_r1.wait_recv()
        cross[(last, 1)].start()
        c_l0.wait_recv()
        cross[(1, 0)].start()
    with jax.named_scope("norm_near2"):
        norm(xbuf.at[last, 0], 0, 0, 1)
        norm(xbuf.at[1, 0], 1, 0, 0)
        cross[(last, 1)].wait_recv()
        cross[(1, 0)].wait_recv()
        norm(xbuf.at[last, 1], 0, 1, 1)
        norm(xbuf.at[1, 1], 1, 1, 0)
    ids_wait(last)
    ids_wait(1)
    tables(last, 0)
    with jax.named_scope("far_wait"):
        f_r.wait_recv()
        cross[(2, 0)].start()
        f_l.wait_recv()
        cross[(2, 1)].start()
    tables(1, 1)
    with jax.named_scope("norm_far"):
        norm(xbuf.at[2, 0], 0, 0, 0)
        norm(xbuf.at[2, 0], 0, 0, 1)
    with jax.named_scope("far_cross_wait"):
        ids_wait(2)
        cross[(2, 0)].wait_recv()
        cross[(2, 1)].wait_recv()
    with jax.named_scope("norm_far2"):
        norm(xbuf.at[2, 1], 0, 1, 0)
        norm(xbuf.at[2, 1], 0, 1, 1)
    tables(2, 0)

    def refill(e):
        @pl.when(e < local_experts - RING // 2)
        def _():
            start_gate_up(e + RING // 2)

        @pl.when(e >= local_experts - RING // 2)
        def _():
            n = 2 * (e - (local_experts - RING // 2))
            start_down(n)
            start_down(n + 1)

    def expert_rest(e, carry):
        with jax.named_scope("gate_up_rest"):
            gate_up_rows(e, rest_rows)
            split_gates(e)
        refill(e)
        return carry

    def expert_all(e, carry):
        slot = 2 * lax.rem(e, RING // 2)
        with jax.named_scope("gate_up_wait"):
            wait_slot(slot)
            wait_slot(slot + 1)
        with jax.named_scope("gate_up"):
            gate_up_rows(e, all_rows)
        refill(e)
        return carry

    lax.fori_loop(0, RING // 2, expert_rest, 0)
    lax.fori_loop(RING // 2, local_experts, expert_all, 0)

    def cross_copy(n, r):
        return remote(ps.at[n, 1, r], d2d.at[n, r], d2d_s.at[n, r], d2d_r.at[n, r], peer)

    def far_copies(n):
        return (
            remote(ps.at[n, 0, 2, 0], far.at[n, 0], far_s.at[n, 0], far_r.at[n, 0], right),
            remote(ps.at[n, 0, 2, 1], far.at[n, 1], far_s.at[n, 1], far_r.at[n, 1], left),
        )

    def near_copies(n):
        return (
            remote(ps.at[n, 0, 1, 1], fin.at[n, 0, 1], fin_s.at[n, 0, 1], fin_r.at[n, 0, 1], right),
            remote(ps.at[n, 0, last, 0], fin.at[n, 1, 0], fin_s.at[n, 1, 0], fin_r.at[n, 1, 0], left),
        )

    def sum_copies(n):
        return (
            remote(ps.at[n, 0, 1, 0], fin.at[n, 0, 0], fin_s.at[n, 0, 0], fin_r.at[n, 0, 0], right),
            remote(ps.at[n, 0, last, 1], fin.at[n, 1, 1], fin_s.at[n, 1, 1], fin_r.at[n, 1, 1], left),
        )

    far_first = (2, 1, last, 0)

    def stage1(n):
        for r in far_first:
            with jax.named_scope("cross_wait"):
                cross_copy(n, r).wait_recv()
            ps[n, 0, r] = ps[n, 0, r] + d2d[n, r]
            if r == 1:
                for c in far_copies(n):
                    c.start()
            if r == last:
                for c in near_copies(n):
                    c.start()

    def chunk(n, carry):
        with jax.named_scope("down_wait"):
            wait_slot(n)
        with jax.named_scope("down"):
            for e in range(local_experts):
                y = dot(act[e], wbuf[n, e]).astype(BF16)
                for r in range(chips):
                    base = r * pair_cap
                    both = y[base + 32 : base + 48]
                    for q in range(2):
                        row = e * own_cap
                        ybuf[r, q, row : row + 16, :] = y[base + 16 * q : base + 16 * (q + 1)]
                        ybuf[r, q, row + 16 : row + 32, :] = both
        @pl.when(n > 0)
        def _():
            stage1(n - 1)

        with jax.named_scope("combine"):
            for r in far_first:
                for q in (1, 0):
                    parts = dot(a3[r, q], ybuf[r, q])
                    total = parts[0:tokens] + (parts[tokens : 2 * tokens] + parts[2 * tokens : 3 * tokens])
                    for h in range(2):
                        ps[n, q, r, h] = total[:, h * LANES : (h + 1) * LANES]
        for r in far_first:
            cross_copy(n, r).start()
        return carry

    def stage2(n, carry):
        from_left, from_right = far_copies(n)
        to_right, to_left = sum_copies(n)
        from_left.wait_recv()
        ps[n, 0, 1, 0] = ps[n, 0, 1, 0] + far[n, 0]
        to_right.start()
        from_right.wait_recv()
        ps[n, 0, last, 1] = ps[n, 0, last, 1] + far[n, 1]
        to_left.start()
        return carry

    lax.fori_loop(0, chunks, chunk, 0)
    stage1(chunks - 1)
    with jax.named_scope("stage2"):
        lax.fori_loop(0, chunks, stage2, 0)

    def final(n, carry):
        for c in near_copies(n) + sum_copies(n):
            c.wait_recv()
        for h in range(2):
            cols = pl.ds(pl.multiple_of(n * COLS + h * LANES, LANES), LANES)
            total = ps[n, 0, 0, h] + fin[n, 0, h] + fin[n, 1, h]
            out_ref[:, cols] = (x_ref[:, cols].astype(F32) + total).astype(BF16)
        return carry

    with jax.named_scope("final"):
        lax.fori_loop(0, chunks, final, 0)

    def drain(n, carry):
        for r in range(chips):
            cross_copy(n, r).wait_send()
        for c in far_copies(n) + near_copies(n) + sum_copies(n):
            c.wait_send()
        return carry

    lax.fori_loop(0, chunks, drain, 0)
    for c in [c_r0, c_l1, c_r1, c_l0, c_p, f_r, f_l] + list(ids_c.values()) + list(cross.values()):
        c.wait_send()


def solution(mesh):
    group = mesh.shape["ep"]
    chips = group // 2

    def local_block(x_in, norm_gain, w_router, expert_ids, w_gate, w_up, w_down):
        tokens, hidden = x_in.shape
        experts = w_router.shape[1]
        top_k = expert_ids.shape[1]
        local_experts, _, ff = w_gate.shape
        cap = 2 * tokens * top_k // experts
        assert cap == 24 and chips == RING // 2
        chunks = hidden // COLS
        wg = w_gate.reshape(local_experts, 2, hidden // 2, ff)
        wu = w_up.reshape(local_experts, 2, hidden // 2, ff)
        vmem = pl.BlockSpec(memory_space=pltpu.VMEM)
        hbm = pl.BlockSpec(memory_space=pl.ANY)
        dma = pltpu.SemaphoreType.DMA
        return pl.pallas_call(
            moe_kernel,
            out_shape=jax.ShapeDtypeStruct((tokens, hidden), BF16),
            in_specs=[hbm] * 7,
            out_specs=vmem,
            scratch_shapes=[
                pltpu.VMEM((tokens, hidden), BF16),
                pltpu.VMEM((hidden // LANES, LANES), BF16),
                pltpu.VMEM((experts, hidden), BF16),
                pltpu.VMEM((top_k, tokens), jnp.int32),
                pltpu.VMEM((RING, local_experts, ff, COLS), BF16),
                pltpu.VMEM((chips, 2, tokens, hidden), BF16),
                pltpu.VMEM((2, 2 * LANES, hidden), BF16),
                pltpu.VMEM((local_experts, group * cap, hidden), BF16),
                pltpu.VMEM((local_experts, group * cap, ff), BF16),
                pltpu.VMEM((local_experts * 48, 2 * LANES), BF16),
                pltpu.VMEM((chips, 2, local_experts * 32, LANES), F32),
                pltpu.VMEM((chips, 2, 3 * tokens, local_experts * 32), BF16),
                pltpu.VMEM((chips, 2, local_experts * 32, COLS), BF16),
                pltpu.VMEM((chunks, 2, chips, 2, tokens, LANES), F32),
                pltpu.VMEM((chunks, chips, 2, tokens, LANES), F32),
                pltpu.VMEM((chunks, 2, tokens, LANES), F32),
                pltpu.VMEM((chunks, 2, 2, tokens, LANES), F32),
                pltpu.VMEM((chips, 2, top_k, LANES), F32),
                pltpu.VMEM((experts, 2 * LANES), F32),
                pltpu.VMEM((experts, 2 * LANES), F32),
                dma((4,)), dma((RING,)),
                dma((chips, 2)), dma((chips, 2)),
                dma((13,)), dma((chips, 2, 2)),
                dma((chunks, chips)), dma((chunks, chips)),
                dma((chunks, 2)), dma((chunks, 2)),
                dma((chunks, 2, 2)), dma((chunks, 2, 2)),
            ],
            compiler_params=pltpu.CompilerParams(
                collective_id=0, has_side_effects=True, vmem_limit_bytes=67043328
            ),
        )(x_in, norm_gain.reshape(hidden // LANES, LANES), w_router.T, expert_ids.T, wg, wu, w_down)

    tok_spec = P(("dp", "ep"), None)
    expert_spec = P("ep", None, None)
    return jax.shard_map(local_block, mesh=mesh, in_specs=(tok_spec, P(None), P(None, None), tok_spec, expert_spec, expert_spec, expert_spec), out_specs=tok_spec, check_vma=False)
```

```python
import functools

import jax
import jax.numpy as jnp
from jax import lax
from jax.experimental import pallas as pl
from jax.experimental.pallas import tpu as pltpu
from jax.sharding import PartitionSpec as P

EPS = 1e-6
F32 = jnp.float32
BF16 = jnp.bfloat16
COLS = 256
LANES = 128
RING = 8


def dot(a, b):
    return jnp.dot(a, b, preferred_element_type=F32)


def moe_kernel(
    x_hbm, gain_hbm, wr_hbm, ids_hbm, wg_ref, wu_ref, wd_ref, out_hbm,
    x_ref, gain_ref, wr_ref, ids_ref,
    out_ref, wbuf, xbuf, hbuf, xe, act, oh, gates, a3, ybuf, ps, d2d, far, fin, ids_all, place, soft,
    in_sem, out_sem, wsem, ids_s, ids_r, link_s, cross_s, ag_r, sum_s, d2d_r, far_r, fin_r,
):
    tokens, hidden = x_ref.shape
    local_experts = act.shape[0]
    experts = wr_ref.shape[0]
    chips = xbuf.shape[0]
    half = tokens // 2
    pair_cap = oh.shape[1] // local_experts
    own_cap = 2 * pair_cap // 3
    chunks = hidden // COLS

    me = lax.axis_index("ep")
    chip, core = me // 2, lax.rem(me, 2)

    def device(r, q):
        return {"ep": lax.rem(chip + r, chips) * 2 + (lax.rem(core + q, 2))}

    last = chips - 1
    far_first = (2, 1, last, 0)
    right, left, peer = device(1, 0), device(chips - 1, 0), device(0, 1)

    def remote(src, dst, send, recv, to):
        return pltpu.make_async_remote_copy(
            src_ref=src, dst_ref=dst, send_sem=send, recv_sem=recv,
            device_id=to, device_id_type=pl.DeviceIdType.MESH,
        )

    def start_gate_up(e, parts=range(4)):
        slot = 2 * (e % (RING // 2))
        for n in parts:
            for k, w in enumerate((wg_ref, wu_ref)):
                pltpu.make_async_copy(
                    w.at[e, :, :, pl.ds(n * COLS, COLS)], wbuf.at[slot + k, pl.ds(2 * n, 2)], wsem.at[slot + k]
                ).start()

    def chunk_slot(n):
        return 2 * (n % (RING // 2)) + n // (RING // 2)

    def start_down(n, parts=range(4)):
        for m in parts:
            pltpu.make_async_copy(
                wd_ref.at[pl.ds(2 * m, 2), :, pl.ds(n * COLS, COLS)], wbuf.at[chunk_slot(n), pl.ds(2 * m, 2)], wsem.at[chunk_slot(n)]
            ).start()

    def wait_bytes(ref, sem):
        pltpu.make_async_copy(ref, ref, sem).wait()

    def wait_slot(slot):
        wait_bytes(wbuf.at[slot], wsem.at[slot])

    barrier = pltpu.get_barrier_semaphore()
    others = [(r, q) for r in range(chips) for q in range(2) if (r, q) != (0, 0)]
    for r, q in others:
        pl.semaphore_signal(barrier, inc=1, device_id=device(r, q), device_id_type=pl.DeviceIdType.MESH)
    inputs = [
        pltpu.make_async_copy(a, b, in_sem.at[k])
        for k, (a, b) in enumerate(((ids_hbm, ids_ref), (x_hbm, x_ref), (gain_hbm, gain_ref), (wr_hbm, wr_ref)))
    ]
    for c in inputs:
        c.start()

    ids_all[0, 0] = jnp.full(ids_all.shape[2:], -1.0, F32)
    with jax.named_scope("inputs"):
        for c in inputs:
            c.wait()
    ids_all[0, 0, :, 0:tokens] = ids_ref[...].astype(F32)
    for e in range(RING // 2):
        start_gate_up(e)
    with jax.named_scope("barrier"):
        pl.semaphore_wait(barrier, len(others))

    top, bot = pl.ds(0, half), pl.ds(half, half)
    c_r0 = remote(x_ref.at[top], xbuf.at[last, 0, top], link_s, ag_r.at[0], right)
    c_l1 = remote(x_ref.at[bot], xbuf.at[1, 0, bot], link_s, ag_r.at[1], left)
    c_r1 = remote(x_ref.at[bot], xbuf.at[last, 0, bot], link_s, ag_r.at[2], right)
    c_l0 = remote(x_ref.at[top], xbuf.at[1, 0, top], link_s, ag_r.at[3], left)
    f_r = remote(xbuf.at[last, 0, top], xbuf.at[2, 0, top], link_s, ag_r.at[4], right)
    f_l = remote(xbuf.at[1, 0, bot], xbuf.at[2, 0, bot], link_s, ag_r.at[5], left)
    c_p = remote(x_ref, xbuf.at[0, 1], cross_s, ag_r.at[6], peer)

    def send_ids(r, q):
        back = (chips - r) % chips
        near = int(r == 0)
        remote(ids_all.at[0, 0], ids_all.at[back, q], ids_s.at[near], ids_r.at[near], device(r, q)).start()

    send_ids(0, 1)
    c_p.start()
    for r, q in others:
        if r > 0:
            send_ids(r, q)
    for c in (c_r0, c_l1, c_r1, c_l0):
        c.start()
    cross = {}
    for r, h, k in ((last, 0, 7), (1, 1, 8), (last, 1, 9), (1, 0, 10), (2, 0, 11), (2, 1, 11)):
        rows = (top, bot)[h]
        cross[(r, h)] = remote(xbuf.at[r, 0, rows], xbuf.at[r, 1, rows], cross_s, ag_r.at[k], peer)

    for k in range(hbuf.shape[0]):
        for q in range(2):
            hbuf[k, q * LANES + tokens : (q + 1) * LANES, :] = jnp.zeros((LANES - tokens, hidden), BF16)
    gain = jnp.concatenate([gain_ref[k : k + 1, :] for k in range(gain_ref.shape[0])], axis=1).astype(F32)
    tri = (
        lax.broadcasted_iota(jnp.int32, (LANES, LANES), 0) < lax.broadcasted_iota(jnp.int32, (LANES, LANES), 1)
    ).astype(BF16)

    def norm(src, k, q, h):
        for g in range(half // 16):
            row = h * half + g * 16
            v = src[row : row + 16, :].astype(F32)
            ms = jnp.mean(v * v, axis=-1, keepdims=True)
            hbuf[k, q * LANES + row : q * LANES + row + 16, :] = (v * lax.rsqrt(ms + EPS) * gain).astype(BF16)

    def slots(r):
        first_expert = (me * local_experts).astype(F32)
        eid = lax.broadcasted_iota(jnp.int32, (local_experts, LANES), 0).astype(F32) + first_expert
        rows = []
        for q in range(2):
            ids = ids_all[r, q]
            hit = eid == ids[0:1, :]
            for j in range(1, ids.shape[0]):
                hit = hit | (eid == ids[j : j + 1, :])
            pos = dot(jnp.where(hit, 1.0, 0.0).astype(BF16), tri)
            first = pos < 15.5
            place[r, q] = jnp.where(hit, jnp.where(first, pos, pos + 8.0 * q), -1.0)
            rows.append(jnp.where(hit, jnp.where(first, pos + 16.0 * q, pos + (16.0 + 8.0 * q)), -1.0))
        pair = jnp.concatenate(rows, axis=1)
        slot = lax.broadcasted_iota(jnp.int32, (pair_cap, 2 * LANES), 0).astype(F32)
        for e in range(local_experts):
            oh[r, pl.ds(e * pair_cap, pair_cap), :] = jnp.where(slot == pair[e : e + 1, :], 1.0, 0.0).astype(BF16)

    def gating(r, k):
        logits = lax.dot_general(
            wr_ref[...], hbuf[k], (((1,), (1,)), ((), ())), preferred_element_type=F32
        )
        shifted = jnp.exp(logits - jnp.max(logits, axis=0, keepdims=True))
        prob = shifted / jnp.sum(shifted, axis=0, keepdims=True)
        ids = jnp.concatenate([ids_all[r, 0], ids_all[r, 1]], axis=1)
        eid = lax.broadcasted_iota(jnp.int32, prob.shape, 0).astype(F32)
        chosen = eid == ids[0:1, :]
        for j in range(1, ids.shape[0]):
            chosen = chosen | (eid == ids[j : j + 1, :])
        picked = jnp.where(chosen, prob, 0.0)
        soft[r] = jnp.where(chosen, picked / jnp.sum(picked, axis=0, keepdims=True), 0.0)
        gate = soft[r, pl.ds(pl.multiple_of(me * local_experts, local_experts), local_experts), :]
        slot = lax.broadcasted_iota(jnp.int32, (own_cap, LANES), 0).astype(F32)
        for q in range(2):
            own = place[r, q]
            for e in range(local_experts):
                gates[r, q, pl.ds(e * own_cap, own_cap), :] = jnp.where(
                    slot == own[e : e + 1, :], gate[e : e + 1, q * LANES : (q + 1) * LANES], 0.0
                )

    def gather(r, k):
        for n in range(hidden // COLS):
            cols = slice(n * COLS, (n + 1) * COLS)
            res = dot(oh[r], hbuf[k, :, cols]).astype(BF16)
            for e in range(local_experts):
                xe[e, r * pair_cap : (r + 1) * pair_cap, cols] = res[e * pair_cap : (e + 1) * pair_cap]

    def split_gates(r):
        for q in range(2):
            gt = gates[r, q].T[0:tokens]
            hi = gt.astype(BF16)
            rest = gt - hi.astype(F32)
            mid = rest.astype(BF16)
            low = (rest - mid.astype(F32)).astype(BF16)
            for p, part in enumerate((hi, mid, low)):
                a3[r, q, pl.ds(p * tokens, tokens), :] = part

    own_ids, other_ids = ids_all.at[0, 1], ids_all.at[pl.ds(1, chips - 1)]

    def gate_up_rows(e, rows, after=lambda n: None):
        slot = 2 * (e % (RING // 2))
        data = xe[e, rows, :]
        for n in range(4):
            g = dot(data, wbuf[slot, 2 * n : 2 * n + 2].reshape(hidden, COLS))
            u = dot(data, wbuf[slot + 1, 2 * n : 2 * n + 2].reshape(hidden, COLS))
            act[e, rows, n * COLS : (n + 1) * COLS] = (g * jax.nn.sigmoid(g) * u).astype(BF16)
            after(n)

    own_rows = pl.ds(0, pair_cap)
    rest_rows = pl.ds(pair_cap, (chips - 1) * pair_cap)
    all_rows = pl.ds(0, chips * pair_cap)

    def own_pass(e, carry):
        with jax.named_scope("own_pass"):
            wait_slot(2 * e)
            wait_slot(2 * e + 1)
            gate_up_rows(e, own_rows)
        return carry

    with jax.named_scope("norm_own"):
        norm(x_ref, 0, 0, 0)
        norm(x_ref, 0, 0, 1)
    with jax.named_scope("own_wait"):
        wait_bytes(own_ids, ids_r.at[1])
        c_p.wait_recv()
    with jax.named_scope("prep_own"):
        norm(xbuf.at[0, 1], 0, 1, 0)
        norm(xbuf.at[0, 1], 0, 1, 1)
        slots(0)
        gather(0, 0)
        gating(0, 0)
    lax.fori_loop(0, 1, own_pass, 0)
    with jax.named_scope("slots"):
        wait_bytes(other_ids, ids_r.at[0])
        for r in (last, 1, 2):
            slots(r)
    lax.fori_loop(1, 2, own_pass, 0)
    with jax.named_scope("near_wait"):
        c_r0.wait_recv()
        f_r.start()
        cross[(last, 0)].start()
        c_l1.wait_recv()
        f_l.start()
        cross[(1, 1)].start()
    with jax.named_scope("norm_near"):
        norm(xbuf.at[last, 0], 0, 0, 0)
        norm(xbuf.at[1, 0], 1, 0, 1)
        cross[(last, 0)].wait_recv()
        cross[(1, 1)].wait_recv()
        norm(xbuf.at[last, 1], 0, 1, 0)
        norm(xbuf.at[1, 1], 1, 1, 1)
    lax.fori_loop(2, RING // 2, own_pass, 0)
    with jax.named_scope("near_wait2"):
        c_r1.wait_recv()
        cross[(last, 1)].start()
        c_l0.wait_recv()
        cross[(1, 0)].start()
    with jax.named_scope("norm_near2"):
        norm(xbuf.at[last, 0], 0, 0, 1)
        norm(xbuf.at[1, 0], 1, 0, 0)
        cross[(last, 1)].wait_recv()
        cross[(1, 0)].wait_recv()
        norm(xbuf.at[last, 1], 0, 1, 1)
        norm(xbuf.at[1, 1], 1, 1, 0)
    with jax.named_scope("gather_near"):
        gather(last, 0)
        gather(1, 1)
    with jax.named_scope("far_wait"):
        f_r.wait_recv()
        cross[(2, 0)].start()
        f_l.wait_recv()
        cross[(2, 1)].start()
    with jax.named_scope("gating_near"):
        gating(last, 0)
        gating(1, 1)
    with jax.named_scope("norm_far"):
        norm(xbuf.at[2, 0], 0, 0, 0)
        norm(xbuf.at[2, 0], 0, 0, 1)
    with jax.named_scope("far_cross_wait"):
        wait_bytes(xbuf.at[2, 1], ag_r.at[11])
    with jax.named_scope("norm_far2"):
        norm(xbuf.at[2, 1], 0, 1, 0)
        norm(xbuf.at[2, 1], 0, 1, 1)
    with jax.named_scope("gather_far"):
        gather(2, 0)

    def refill(e):
        def after(n):
            if e < local_experts - RING // 2:
                start_gate_up(e + RING // 2, (n,))
            else:
                start_down(e - (local_experts - RING // 2), (n,))
        return after

    with jax.named_scope("gate_up_rest"):
        for e in range(RING // 2):
            gate_up_rows(e, rest_rows, refill(e))
            if e == 0:
                gating(2, 0)
            split_gates(far_first[chips - 1 - e])
    for e in range(RING // 2, local_experts):
        slot = 2 * (e % (RING // 2))
        with jax.named_scope("gate_up_wait"):
            wait_slot(slot)
            wait_slot(slot + 1)
        with jax.named_scope("gate_up"):
            gate_up_rows(e, all_rows, refill(e))
    for n in range(RING // 2, chunks):
        start_down(n)

    def cross_copy(n):
        return remote(ps.at[n, 1], d2d.at[n], sum_s.at[0], d2d_r.at[n], peer)

    def far_copies(n):
        return (
            remote(ps.at[n, 0, 2, 0], far.at[n, 0], sum_s.at[1], far_r.at[n], right),
            remote(ps.at[n, 0, 2, 1], far.at[n, 1], sum_s.at[1], far_r.at[n], left),
        )

    def near_copies(n):
        return (
            remote(ps.at[n, 0, 1, 1], fin.at[n, 0, 1], sum_s.at[2], fin_r.at[n], right),
            remote(ps.at[n, 0, last, 0], fin.at[n, 1, 0], sum_s.at[2], fin_r.at[n], left),
        )

    def sum_copies(n):
        return (
            remote(ps.at[n, 0, 1, 0], fin.at[n, 0, 0], sum_s.at[2], fin_r.at[n], right),
            remote(ps.at[n, 0, last, 1], fin.at[n, 1, 1], sum_s.at[2], fin_r.at[n], left),
        )

    def stage1(n):
        with jax.named_scope("cross_wait"):
            cross_copy(n).wait_recv()
        for r in far_first:
            ps[n, 0, r] = ps[n, 0, r] + d2d[n, r]
            if r == 1:
                for c in far_copies(n):
                    c.start()
            if r == last:
                for c in near_copies(n):
                    c.start()

    def chunk(n, carry):
        with jax.named_scope("down_wait"):
            wslot = 2 * lax.rem(n, RING // 2) + n // (RING // 2)
            wait_slot(wslot)
        with jax.named_scope("down"):
            for e in range(local_experts):
                y = dot(act[e], wbuf[wslot, e]).astype(BF16)
                for r in range(chips):
                    base = r * pair_cap
                    both = y[base + 32 : base + 48]
                    for q in range(2):
                        row = e * own_cap
                        ybuf[r, q, row : row + 16, :] = y[base + 16 * q : base + 16 * (q + 1)]
                        ybuf[r, q, row + 16 : row + 32, :] = both

        @pl.when(n > 0)
        def _():
            stage1(n - 1)

        with jax.named_scope("combine"):
            for r in far_first:
                for q in (1, 0):
                    parts = dot(a3[r, q], ybuf[r, q])
                    total = parts[0:tokens] + (parts[tokens : 2 * tokens] + parts[2 * tokens : 3 * tokens])
                    for h in range(2):
                        ps[n, q, r, h] = total[:, h * LANES : (h + 1) * LANES]
        cross_copy(n).start()
        return carry

    lax.fori_loop(0, chunks, chunk, 0)
    wait_bytes(act.at[pl.ds(0, 3)], link_s)
    wait_bytes(xbuf.at[pl.ds(0, 2)], cross_s)
    wait_bytes(own_ids, ids_s.at[1])
    wait_bytes(other_ids, ids_s.at[0])
    stage1(chunks - 1)

    def stage2(n, carry):
        to_right, to_left = sum_copies(n)
        with jax.named_scope("far_sum_wait"):
            wait_bytes(far.at[n], far_r.at[n])
        ps[n, 0, 1, 0] = ps[n, 0, 1, 0] + far[n, 0]
        ps[n, 0, last, 1] = ps[n, 0, last, 1] + far[n, 1]
        to_right.start()
        to_left.start()
        return carry

    with jax.named_scope("stage2"):
        lax.fori_loop(0, chunks, stage2, 0)

    def final(n, carry):
        with jax.named_scope("final_wait"):
            wait_bytes(fin.at[n], fin_r.at[n])
        for h in range(2):
            cols = pl.ds(pl.multiple_of(n * COLS + h * LANES, LANES), LANES)
            total = ps[n, 0, 0, h] + fin[n, 0, h] + fin[n, 1, h]
            out_ref[:, cols] = (x_ref[:, cols].astype(F32) + total).astype(BF16)
        cols = pl.ds(pl.multiple_of(n * COLS, COLS), COLS)
        pltpu.make_async_copy(out_ref.at[:, cols], out_hbm.at[:, cols], out_sem).start()
        return carry

    with jax.named_scope("final"):
        lax.fori_loop(0, chunks, final, 0)
    with jax.named_scope("send_wait"):
        wait_bytes(d2d, sum_s.at[0])
        wait_bytes(far, sum_s.at[1])
        wait_bytes(fin, sum_s.at[2])
        wait_bytes(out_ref, out_sem)


def solution(mesh):
    group = mesh.shape["ep"]
    chips = group // 2

    def local_block(x_in, norm_gain, w_router, expert_ids, w_gate, w_up, w_down):
        tokens, hidden = x_in.shape
        experts = w_router.shape[1]
        top_k = expert_ids.shape[1]
        local_experts, _, ff = w_gate.shape
        cap = 2 * tokens * top_k // experts
        assert cap == 24 and chips == RING // 2
        chunks = hidden // COLS
        wg = w_gate.reshape(local_experts, 2, hidden // 2, ff)
        wu = w_up.reshape(local_experts, 2, hidden // 2, ff)
        hbm = pl.BlockSpec(memory_space=pl.ANY)
        dma = pltpu.SemaphoreType.DMA
        return pl.pallas_call(
            moe_kernel,
            out_shape=jax.ShapeDtypeStruct((tokens, hidden), BF16),
            in_specs=[hbm] * 7,
            out_specs=hbm,
            scratch_shapes=[
                pltpu.VMEM((tokens, hidden), BF16),
                pltpu.VMEM((hidden // LANES, LANES), BF16),
                pltpu.VMEM((experts, hidden), BF16),
                pltpu.VMEM((top_k, tokens), jnp.int32),
                pltpu.VMEM((tokens, hidden), BF16),
                pltpu.VMEM((RING, local_experts, ff, COLS), BF16),
                pltpu.VMEM((chips, 2, tokens, hidden), BF16),
                pltpu.VMEM((2, 2 * LANES, hidden), BF16),
                pltpu.VMEM((local_experts, group * cap, hidden), BF16),
                pltpu.VMEM((local_experts, group * cap, ff), BF16),
                pltpu.VMEM((chips, local_experts * 48, 2 * LANES), BF16),
                pltpu.VMEM((chips, 2, local_experts * 32, LANES), F32),
                pltpu.VMEM((chips, 2, 3 * tokens, local_experts * 32), BF16),
                pltpu.VMEM((chips, 2, local_experts * 32, COLS), BF16),
                pltpu.VMEM((chunks, 2, chips, 2, tokens, LANES), F32),
                pltpu.VMEM((chunks, chips, 2, tokens, LANES), F32),
                pltpu.VMEM((chunks, 2, tokens, LANES), F32),
                pltpu.VMEM((chunks, 2, 2, tokens, LANES), F32),
                pltpu.VMEM((chips, 2, top_k, LANES), F32),
                pltpu.VMEM((chips, 2, local_experts, LANES), F32),
                pltpu.VMEM((chips, experts, 2 * LANES), F32),
                dma((4,)), dma, dma((RING,)), dma((2,)), dma((2,)),
                dma, dma, dma((12,)), dma((3,)), dma((chunks,)), dma((chunks,)), dma((chunks,)),
            ],
            compiler_params=pltpu.CompilerParams(
                collective_id=0, has_side_effects=True, vmem_limit_bytes=67043328
            ),
        )(x_in, norm_gain.reshape(hidden // LANES, LANES), w_router.T, expert_ids.T, wg, wu, w_down)

    tok_spec = P(("dp", "ep"), None)
    expert_spec = P("ep", None, None)
    return jax.shard_map(local_block, mesh=mesh, in_specs=(tok_spec, P(None), P(None, None), tok_spec, expert_spec, expert_spec, expert_spec), out_specs=tok_spec, check_vma=False)
```

```python
import functools

import jax
import jax.numpy as jnp
from jax import lax
from jax.experimental import pallas as pl
from jax.experimental.pallas import tpu as pltpu
from jax.sharding import PartitionSpec as P

EPS = 1e-6
F32 = jnp.float32
BF16 = jnp.bfloat16
COLS = 256
LANES = 128
RING = 8


def dot(a, b):
    return jnp.dot(a, b, preferred_element_type=F32)


def moe_kernel(
    x_hbm, gain_hbm, wr_hbm, ids_hbm, wg_ref, wu_ref, wd_ref, out_hbm,
    x_ref, gain_ref, wr_ref, ids_ref,
    wbuf, xbuf, hbuf, xe, act, oh, gates, a3, ybuf, ps, d2d, far, fin, ids_all, place, soft,
    in_sem, wsem, ids_s, ids_r, link_s, cross_s, ag_r, sum_s, d2d_r, far_r, fin_r,
):
    tokens, hidden = x_ref.shape
    local_experts = act.shape[0]
    experts = wr_ref.shape[0]
    chips = xbuf.shape[0]
    half = tokens // 2
    pair_cap = oh.shape[1] // local_experts
    own_cap = 2 * pair_cap // 3
    chunks = hidden // COLS

    me = lax.axis_index("ep")
    chip, core = me // 2, lax.rem(me, 2)

    def device(r, q):
        return {"ep": lax.rem(chip + r, chips) * 2 + (lax.rem(core + q, 2))}

    last = chips - 1
    far_first = (2, 1, last, 0)
    right, left, peer = device(1, 0), device(chips - 1, 0), device(0, 1)

    def remote(src, dst, send, recv, to):
        return pltpu.make_async_remote_copy(
            src_ref=src, dst_ref=dst, send_sem=send, recv_sem=recv,
            device_id=to, device_id_type=pl.DeviceIdType.MESH,
        )

    def start_gate_up(e, parts=range(4)):
        slot = 2 * (e % (RING // 2))
        for n in parts:
            for k, w in enumerate((wg_ref, wu_ref)):
                pltpu.make_async_copy(
                    w.at[e, :, :, pl.ds(n * COLS, COLS)], wbuf.at[slot + k, pl.ds(2 * n, 2)], wsem.at[slot + k]
                ).start()

    def chunk_slot(n):
        return 2 * (n % (RING // 2)) + n // (RING // 2)

    def start_down(n, parts=range(4)):
        for m in parts:
            pltpu.make_async_copy(
                wd_ref.at[pl.ds(2 * m, 2), :, pl.ds(n * COLS, COLS)], wbuf.at[chunk_slot(n), pl.ds(2 * m, 2)], wsem.at[chunk_slot(n)]
            ).start()

    def wait_bytes(ref, sem):
        pltpu.make_async_copy(ref, ref, sem).wait()

    def wait_slot(slot):
        wait_bytes(wbuf.at[slot], wsem.at[slot])

    barrier = pltpu.get_barrier_semaphore()
    others = [(r, q) for r in range(chips) for q in range(2) if (r, q) != (0, 0)]
    for r, q in others:
        pl.semaphore_signal(barrier, inc=1, device_id=device(r, q), device_id_type=pl.DeviceIdType.MESH)
    inputs = [
        pltpu.make_async_copy(a, b, in_sem.at[k])
        for k, (a, b) in enumerate(((ids_hbm, ids_ref), (x_hbm, x_ref), (gain_hbm, gain_ref), (wr_hbm, wr_ref)))
    ]
    for c in inputs:
        c.start()

    ids_all[0, 0] = jnp.full(ids_all.shape[2:], -1.0, F32)
    with jax.named_scope("inputs"):
        for c in inputs:
            c.wait()
    ids_all[0, 0, :, 0:tokens] = ids_ref[...].astype(F32)
    for e in range(RING // 2):
        start_gate_up(e)
    with jax.named_scope("barrier"):
        pl.semaphore_wait(barrier, len(others))

    top, bot = pl.ds(0, half), pl.ds(half, half)
    c_r0 = remote(x_ref.at[top], xbuf.at[last, 0, top], link_s, ag_r.at[0], right)
    c_l1 = remote(x_ref.at[bot], xbuf.at[1, 0, bot], link_s, ag_r.at[1], left)
    c_r1 = remote(x_ref.at[bot], xbuf.at[last, 0, bot], link_s, ag_r.at[2], right)
    c_l0 = remote(x_ref.at[top], xbuf.at[1, 0, top], link_s, ag_r.at[3], left)
    f_r = remote(xbuf.at[last, 0, top], xbuf.at[2, 0, top], link_s, ag_r.at[4], right)
    f_l = remote(xbuf.at[1, 0, bot], xbuf.at[2, 0, bot], link_s, ag_r.at[5], left)
    c_p = remote(x_ref, xbuf.at[0, 1], cross_s, ag_r.at[6], peer)

    def send_ids(r, q):
        back = (chips - r) % chips
        near = int(r == 0)
        remote(ids_all.at[0, 0], ids_all.at[back, q], ids_s.at[near], ids_r.at[near], device(r, q)).start()

    send_ids(0, 1)
    c_p.start()
    for r, q in others:
        if r > 0:
            send_ids(r, q)
    for c in (c_r0, c_l1, c_r1, c_l0):
        c.start()
    cross = {}
    for r, h, k in ((last, 0, 7), (1, 1, 8), (last, 1, 9), (1, 0, 10), (2, 0, 11), (2, 1, 11)):
        rows = (top, bot)[h]
        cross[(r, h)] = remote(xbuf.at[r, 0, rows], xbuf.at[r, 1, rows], cross_s, ag_r.at[k], peer)

    for k in range(hbuf.shape[0]):
        for q in range(2):
            hbuf[k, q * LANES + tokens : (q + 1) * LANES, :] = jnp.zeros((LANES - tokens, hidden), BF16)
    gain = jnp.concatenate([gain_ref[k : k + 1, :] for k in range(gain_ref.shape[0])], axis=1).astype(F32)
    tri = (
        lax.broadcasted_iota(jnp.int32, (LANES, LANES), 0) < lax.broadcasted_iota(jnp.int32, (LANES, LANES), 1)
    ).astype(BF16)

    def norm(src, k, q, h):
        for g in range(half // 16):
            row = h * half + g * 16
            v = src[row : row + 16, :].astype(F32)
            ms = jnp.mean(v * v, axis=-1, keepdims=True)
            hbuf[k, q * LANES + row : q * LANES + row + 16, :] = (v * lax.rsqrt(ms + EPS) * gain).astype(BF16)

    def slots(r):
        first_expert = (me * local_experts).astype(F32)
        eid = lax.broadcasted_iota(jnp.int32, (local_experts, LANES), 0).astype(F32) + first_expert
        rows = []
        for q in range(2):
            ids = ids_all[r, q]
            hit = eid == ids[0:1, :]
            for j in range(1, ids.shape[0]):
                hit = hit | (eid == ids[j : j + 1, :])
            pos = dot(jnp.where(hit, 1.0, 0.0).astype(BF16), tri)
            first = pos < 15.5
            place[r, q] = jnp.where(hit, jnp.where(first, pos, pos + 8.0 * q), -1.0)
            rows.append(jnp.where(hit, jnp.where(first, pos + 16.0 * q, pos + (16.0 + 8.0 * q)), -1.0))
        pair = jnp.concatenate(rows, axis=1)
        slot = lax.broadcasted_iota(jnp.int32, (pair_cap, 2 * LANES), 0).astype(F32)
        for e in range(local_experts):
            oh[r, pl.ds(e * pair_cap, pair_cap), :] = jnp.where(slot == pair[e : e + 1, :], 1.0, 0.0).astype(BF16)

    def gating(r, k):
        logits = lax.dot_general(
            wr_ref[...], hbuf[k], (((1,), (1,)), ((), ())), preferred_element_type=F32
        )
        shifted = jnp.exp(logits - jnp.max(logits, axis=0, keepdims=True))
        prob = shifted / jnp.sum(shifted, axis=0, keepdims=True)
        ids = jnp.concatenate([ids_all[r, 0], ids_all[r, 1]], axis=1)
        eid = lax.broadcasted_iota(jnp.int32, prob.shape, 0).astype(F32)
        chosen = eid == ids[0:1, :]
        for j in range(1, ids.shape[0]):
            chosen = chosen | (eid == ids[j : j + 1, :])
        picked = jnp.where(chosen, prob, 0.0)
        soft[r] = jnp.where(chosen, picked / jnp.sum(picked, axis=0, keepdims=True), 0.0)
        gate = soft[r, pl.ds(pl.multiple_of(me * local_experts, local_experts), local_experts), :]
        slot = lax.broadcasted_iota(jnp.int32, (own_cap, LANES), 0).astype(F32)
        for q in range(2):
            own = place[r, q]
            for e in range(local_experts):
                gates[r, q, pl.ds(e * own_cap, own_cap), :] = jnp.where(
                    slot == own[e : e + 1, :], gate[e : e + 1, q * LANES : (q + 1) * LANES], 0.0
                )

    def gather(r, k):
        for n in range(hidden // COLS):
            cols = slice(n * COLS, (n + 1) * COLS)
            res = dot(oh[r], hbuf[k, :, cols]).astype(BF16)
            for e in range(local_experts):
                xe[e, r * pair_cap : (r + 1) * pair_cap, cols] = res[e * pair_cap : (e + 1) * pair_cap]

    def split_gates(r):
        for q in range(2):
            gt = gates[r, q].T[0:tokens]
            hi = gt.astype(BF16)
            rest = gt - hi.astype(F32)
            mid = rest.astype(BF16)
            low = (rest - mid.astype(F32)).astype(BF16)
            for p, part in enumerate((hi, mid, low)):
                a3[r, q, pl.ds(p * tokens, tokens), :] = part

    own_ids, other_ids = ids_all.at[0, 1], ids_all.at[pl.ds(1, chips - 1)]

    def gate_up_rows(e, rows, after=lambda n: None):
        slot = 2 * (e % (RING // 2))
        data = xe[e, rows, :]
        for n in range(4):
            g = dot(data, wbuf[slot, 2 * n : 2 * n + 2].reshape(hidden, COLS))
            u = dot(data, wbuf[slot + 1, 2 * n : 2 * n + 2].reshape(hidden, COLS))
            act[e, rows, n * COLS : (n + 1) * COLS] = (g * jax.nn.sigmoid(g) * u).astype(BF16)
            after(n)

    own_rows = pl.ds(0, pair_cap)
    rest_rows = pl.ds(pair_cap, (chips - 1) * pair_cap)
    all_rows = pl.ds(0, chips * pair_cap)

    def own_pass(e, carry):
        with jax.named_scope("own_pass"):
            wait_slot(2 * e)
            wait_slot(2 * e + 1)
            gate_up_rows(e, own_rows)
        return carry

    with jax.named_scope("norm_own"):
        norm(x_ref, 0, 0, 0)
        norm(x_ref, 0, 0, 1)
    with jax.named_scope("own_wait"):
        wait_bytes(own_ids, ids_r.at[1])
        c_p.wait_recv()
    with jax.named_scope("prep_own"):
        norm(xbuf.at[0, 1], 0, 1, 0)
        norm(xbuf.at[0, 1], 0, 1, 1)
        slots(0)
        gather(0, 0)
        gating(0, 0)
    lax.fori_loop(0, 1, own_pass, 0)
    with jax.named_scope("slots"):
        wait_bytes(other_ids, ids_r.at[0])
        for r in (last, 1, 2):
            slots(r)
    lax.fori_loop(1, 2, own_pass, 0)
    with jax.named_scope("near_wait"):
        c_r0.wait_recv()
        f_r.start()
        cross[(last, 0)].start()
        c_l1.wait_recv()
        f_l.start()
        cross[(1, 1)].start()
    with jax.named_scope("norm_near"):
        norm(xbuf.at[last, 0], 0, 0, 0)
        norm(xbuf.at[1, 0], 1, 0, 1)
        cross[(last, 0)].wait_recv()
        cross[(1, 1)].wait_recv()
        norm(xbuf.at[last, 1], 0, 1, 0)
        norm(xbuf.at[1, 1], 1, 1, 1)
    lax.fori_loop(2, RING // 2, own_pass, 0)
    with jax.named_scope("near_wait2"):
        c_r1.wait_recv()
        cross[(last, 1)].start()
        c_l0.wait_recv()
        cross[(1, 0)].start()
    with jax.named_scope("norm_near2"):
        norm(xbuf.at[last, 0], 0, 0, 1)
        norm(xbuf.at[1, 0], 1, 0, 0)
        cross[(last, 1)].wait_recv()
        cross[(1, 0)].wait_recv()
        norm(xbuf.at[last, 1], 0, 1, 1)
        norm(xbuf.at[1, 1], 1, 1, 0)
    with jax.named_scope("gather_near"):
        gather(last, 0)
        gather(1, 1)
    with jax.named_scope("far_wait"):
        f_r.wait_recv()
        cross[(2, 0)].start()
        f_l.wait_recv()
        cross[(2, 1)].start()
    with jax.named_scope("gating_near"):
        gating(last, 0)
        gating(1, 1)
    with jax.named_scope("norm_far"):
        norm(xbuf.at[2, 0], 0, 0, 0)
        norm(xbuf.at[2, 0], 0, 0, 1)
    with jax.named_scope("far_cross_wait"):
        wait_bytes(xbuf.at[2, 1], ag_r.at[11])
    with jax.named_scope("norm_far2"):
        norm(xbuf.at[2, 1], 0, 1, 0)
        norm(xbuf.at[2, 1], 0, 1, 1)
    with jax.named_scope("gather_far"):
        gather(2, 0)

    def refill(e):
        def after(n):
            if e < local_experts - RING // 2:
                start_gate_up(e + RING // 2, (n,))
            else:
                start_down(e - (local_experts - RING // 2), (n,))
        return after

    with jax.named_scope("gate_up_rest"):
        for e in range(RING // 2):
            gate_up_rows(e, rest_rows, refill(e))
            if e == 0:
                gating(2, 0)
            split_gates(far_first[chips - 1 - e])
    for e in range(RING // 2, local_experts):
        slot = 2 * (e % (RING // 2))
        with jax.named_scope("gate_up_wait"):
            wait_slot(slot)
            wait_slot(slot + 1)
        with jax.named_scope("gate_up"):
            gate_up_rows(e, all_rows, refill(e))
    for n in range(RING // 2, chunks):
        start_down(n)

    def cross_copy(n):
        return remote(ps.at[n, 1], d2d.at[n], sum_s.at[0], d2d_r.at[n], peer)

    def far_copies(n):
        return (
            remote(ps.at[n, 0, 2, 0], far.at[n, 0], sum_s.at[1], far_r.at[n], right),
            remote(ps.at[n, 0, 2, 1], far.at[n, 1], sum_s.at[1], far_r.at[n], left),
        )

    def near_copies(n):
        return (
            remote(ps.at[n, 0, 1, 1], fin.at[n, 0, 1], sum_s.at[2], fin_r.at[n], right),
            remote(ps.at[n, 0, last, 0], fin.at[n, 1, 0], sum_s.at[2], fin_r.at[n], left),
        )

    def sum_copies(n):
        return (
            remote(ps.at[n, 0, 1, 0], fin.at[n, 0, 0], sum_s.at[2], fin_r.at[n], right),
            remote(ps.at[n, 0, last, 1], fin.at[n, 1, 1], sum_s.at[2], fin_r.at[n], left),
        )

    def stage1(n):
        with jax.named_scope("cross_wait"):
            cross_copy(n).wait_recv()
        for r in far_first:
            ps[n, 0, r] = ps[n, 0, r] + d2d[n, r]
            if r == 1:
                for c in far_copies(n):
                    c.start()
            if r == last:
                for c in near_copies(n):
                    c.start()

    def chunk(n, carry):
        with jax.named_scope("down_wait"):
            wslot = 2 * lax.rem(n, RING // 2) + n // (RING // 2)
            wait_slot(wslot)
        with jax.named_scope("down"):
            for e in range(local_experts):
                y = dot(act[e], wbuf[wslot, e]).astype(BF16)
                for r in range(chips):
                    base = r * pair_cap
                    both = y[base + 32 : base + 48]
                    for q in range(2):
                        row = e * own_cap
                        ybuf[r, q, row : row + 16, :] = y[base + 16 * q : base + 16 * (q + 1)]
                        ybuf[r, q, row + 16 : row + 32, :] = both

        @pl.when(n > 0)
        def _():
            stage1(n - 1)

        with jax.named_scope("combine"):
            for r in far_first:
                for q in (1, 0):
                    parts = dot(a3[r, q], ybuf[r, q])
                    total = parts[0:tokens] + (parts[tokens : 2 * tokens] + parts[2 * tokens : 3 * tokens])
                    for h in range(2):
                        ps[n, q, r, h] = total[:, h * LANES : (h + 1) * LANES]
        cross_copy(n).start()
        return carry

    lax.fori_loop(0, chunks, chunk, 0)
    wait_bytes(act.at[pl.ds(0, 3)], link_s)
    wait_bytes(xbuf.at[pl.ds(0, 2)], cross_s)
    wait_bytes(own_ids, ids_s.at[1])
    wait_bytes(other_ids, ids_s.at[0])
    stage1(chunks - 1)

    def stage2(n, carry):
        to_right, to_left = sum_copies(n)
        with jax.named_scope("far_sum_wait"):
            wait_bytes(far.at[n], far_r.at[n])
        ps[n, 0, 1, 0] = ps[n, 0, 1, 0] + far[n, 0]
        ps[n, 0, last, 1] = ps[n, 0, last, 1] + far[n, 1]
        to_right.start()
        to_left.start()
        return carry

    with jax.named_scope("stage2"):
        lax.fori_loop(0, chunks, stage2, 0)

    def final(n, carry):
        with jax.named_scope("final_wait"):
            wait_bytes(fin.at[n], fin_r.at[n])
        for h in range(2):
            cols = pl.ds(pl.multiple_of(n * COLS + h * LANES, LANES), LANES)
            total = ps[n, 0, 0, h] + fin[n, 0, h] + fin[n, 1, h]
            out_hbm[:, cols] = (x_ref[:, cols].astype(F32) + total).astype(BF16)
        return carry

    with jax.named_scope("final"):
        lax.fori_loop(0, chunks, final, 0)
    with jax.named_scope("send_wait"):
        wait_bytes(d2d, sum_s.at[0])
        wait_bytes(far, sum_s.at[1])
        wait_bytes(fin, sum_s.at[2])


def solution(mesh):
    group = mesh.shape["ep"]
    chips = group // 2

    def local_block(x_in, norm_gain, w_router, expert_ids, w_gate, w_up, w_down):
        tokens, hidden = x_in.shape
        experts = w_router.shape[1]
        top_k = expert_ids.shape[1]
        local_experts, _, ff = w_gate.shape
        cap = 2 * tokens * top_k // experts
        assert cap == 24 and chips == RING // 2
        chunks = hidden // COLS
        wg = w_gate.reshape(local_experts, 2, hidden // 2, ff)
        wu = w_up.reshape(local_experts, 2, hidden // 2, ff)
        hbm = pl.BlockSpec(memory_space=pl.ANY)
        dma = pltpu.SemaphoreType.DMA
        return pl.pallas_call(
            moe_kernel,
            out_shape=pltpu.VMEM((tokens, hidden), BF16),
            in_specs=[hbm] * 7,
            out_specs=pl.BlockSpec(memory_space=pltpu.VMEM),
            scratch_shapes=[
                pltpu.VMEM((tokens, hidden), BF16),
                pltpu.VMEM((hidden // LANES, LANES), BF16),
                pltpu.VMEM((experts, hidden), BF16),
                pltpu.VMEM((top_k, tokens), jnp.int32),
                pltpu.VMEM((RING, local_experts, ff, COLS), BF16),
                pltpu.VMEM((chips, 2, tokens, hidden), BF16),
                pltpu.VMEM((2, 2 * LANES, hidden), BF16),
                pltpu.VMEM((local_experts, group * cap, hidden), BF16),
                pltpu.VMEM((local_experts, group * cap, ff), BF16),
                pltpu.VMEM((chips, local_experts * 48, 2 * LANES), BF16),
                pltpu.VMEM((chips, 2, local_experts * 32, LANES), F32),
                pltpu.VMEM((chips, 2, 3 * tokens, local_experts * 32), BF16),
                pltpu.VMEM((chips, 2, local_experts * 32, COLS), BF16),
                pltpu.VMEM((chunks, 2, chips, 2, tokens, LANES), F32),
                pltpu.VMEM((chunks, chips, 2, tokens, LANES), F32),
                pltpu.VMEM((chunks, 2, tokens, LANES), F32),
                pltpu.VMEM((chunks, 2, 2, tokens, LANES), F32),
                pltpu.VMEM((chips, 2, top_k, LANES), F32),
                pltpu.VMEM((chips, 2, local_experts, LANES), F32),
                pltpu.VMEM((chips, experts, 2 * LANES), F32),
                dma((4,)), dma((RING,)), dma((2,)), dma((2,)),
                dma, dma, dma((12,)), dma((3,)), dma((chunks,)), dma((chunks,)), dma((chunks,)),
            ],
            compiler_params=pltpu.CompilerParams(
                collective_id=0, has_side_effects=True, vmem_limit_bytes=66600000
            ),
        )(x_in, norm_gain.reshape(hidden // LANES, LANES), w_router.T, expert_ids.T, wg, wu, w_down)

    tok_spec = P(("dp", "ep"), None)
    expert_spec = P("ep", None, None)
    return jax.shard_map(local_block, mesh=mesh, in_specs=(tok_spec, P(None), P(None, None), tok_spec, expert_spec, expert_spec, expert_spec), out_specs=tok_spec, check_vma=False)
```

```python
import functools

import jax
import jax.numpy as jnp
from jax import lax
from jax.experimental import pallas as pl
from jax.experimental.pallas import tpu as pltpu
from jax.sharding import PartitionSpec as P

EPS = 1e-6
F32 = jnp.float32
BF16 = jnp.bfloat16
COLS = 256
LANES = 128
RING = 8


def dot(a, b):
    return jnp.dot(a, b, preferred_element_type=F32)


def moe_kernel(
    x_hbm, gain_hbm, wr_hbm, ids_hbm, wg_ref, wu_ref, wd_ref, out_hbm,
    x_ref, gain_ref, wr_ref, ids_ref,
    wbuf, xbuf, hbuf, xe, act, oh, gates, a3, ybuf, ps, d2d, far, fin, ids_all, place, soft,
    in_sem, wsem, ids_s, ids_r, link_s, cross_s, ag_r, sum_s, d2d_r, far_r, fin_r,
):
    tokens, hidden = x_ref.shape
    local_experts = act.shape[0]
    experts = wr_ref.shape[0]
    chips = xbuf.shape[0]
    half = tokens // 2
    pair_cap = oh.shape[1] // local_experts
    own_cap = 2 * pair_cap // 3
    chunks = hidden // COLS

    me = lax.axis_index("ep")
    chip, core = me // 2, lax.rem(me, 2)

    def device(r, q):
        return {"ep": lax.rem(chip + r, chips) * 2 + (lax.rem(core + q, 2))}

    last = chips - 1
    far_first = (2, 1, last, 0)
    right, left, peer = device(1, 0), device(chips - 1, 0), device(0, 1)

    def remote(src, dst, send, recv, to):
        return pltpu.make_async_remote_copy(
            src_ref=src, dst_ref=dst, send_sem=send, recv_sem=recv,
            device_id=to, device_id_type=pl.DeviceIdType.MESH,
        )

    def start_gate_up(e, parts=range(4)):
        slot = 2 * (e % (RING // 2))
        for n in parts:
            for k, w in enumerate((wg_ref, wu_ref)):
                pltpu.make_async_copy(
                    w.at[e, :, :, pl.ds(n * COLS, COLS)], wbuf.at[slot + k, pl.ds(2 * n, 2)], wsem.at[slot + k]
                ).start()

    def chunk_slot(n):
        return 2 * (n % (RING // 2)) + n // (RING // 2)

    def start_down(n):
        slot = chunk_slot(n)
        pltpu.make_async_copy(wd_ref.at[:, :, pl.ds(n * COLS, COLS)], wbuf.at[slot], wsem.at[slot]).start()

    def wait_bytes(ref, sem):
        pltpu.make_async_copy(ref, ref, sem).wait()

    def wait_slot(slot):
        wait_bytes(wbuf.at[slot], wsem.at[slot])

    barrier = pltpu.get_barrier_semaphore()
    others = [(r, q) for r in range(chips) for q in range(2) if (r, q) != (0, 0)]
    for r, q in others:
        pl.semaphore_signal(barrier, inc=1, device_id=device(r, q), device_id_type=pl.DeviceIdType.MESH)
    inputs = [
        pltpu.make_async_copy(a, b, in_sem.at[k])
        for k, (a, b) in enumerate(((ids_hbm, ids_ref), (x_hbm, x_ref), (gain_hbm, gain_ref), (wr_hbm, wr_ref)))
    ]
    for c in inputs:
        c.start()

    ids_all[0, 0] = jnp.full(ids_all.shape[2:], -1.0, F32)
    with jax.named_scope("inputs"):
        for c in inputs:
            c.wait()
    ids_all[0, 0, :, 0:tokens] = ids_ref[...].astype(F32)
    for e in range(RING // 2):
        start_gate_up(e)
    with jax.named_scope("barrier"):
        pl.semaphore_wait(barrier, len(others))

    top, bot = pl.ds(0, half), pl.ds(half, half)
    c_r0 = remote(x_ref.at[top], xbuf.at[last, 0, top], link_s, ag_r.at[0], right)
    c_l1 = remote(x_ref.at[bot], xbuf.at[1, 0, bot], link_s, ag_r.at[1], left)
    c_r1 = remote(x_ref.at[bot], xbuf.at[last, 0, bot], link_s, ag_r.at[2], right)
    c_l0 = remote(x_ref.at[top], xbuf.at[1, 0, top], link_s, ag_r.at[3], left)
    f_r = remote(xbuf.at[last, 0, top], xbuf.at[2, 0, top], link_s, ag_r.at[4], right)
    f_l = remote(xbuf.at[1, 0, bot], xbuf.at[2, 0, bot], link_s, ag_r.at[5], left)
    c_p = remote(x_ref, xbuf.at[0, 1], cross_s, ag_r.at[6], peer)

    def send_ids(r, q):
        back = (chips - r) % chips
        near = int(r == 0)
        remote(ids_all.at[0, 0], ids_all.at[back, q], ids_s.at[near], ids_r.at[near], device(r, q)).start()

    send_ids(0, 1)
    c_p.start()
    for r, q in others:
        if r > 0:
            send_ids(r, q)
    for c in (c_r0, c_l1, c_r1, c_l0):
        c.start()
    cross = {}
    for r, h, k in ((last, 0, 7), (1, 1, 8), (last, 1, 9), (1, 0, 10), (2, 0, 11), (2, 1, 11)):
        rows = (top, bot)[h]
        cross[(r, h)] = remote(xbuf.at[r, 0, rows], xbuf.at[r, 1, rows], cross_s, ag_r.at[k], peer)

    for k in range(hbuf.shape[0]):
        for q in range(2):
            hbuf[k, q * LANES + tokens : (q + 1) * LANES, :] = jnp.zeros((LANES - tokens, hidden), BF16)
    gain = jnp.concatenate([gain_ref[k : k + 1, :] for k in range(gain_ref.shape[0])], axis=1).astype(F32)
    tri = (
        lax.broadcasted_iota(jnp.int32, (LANES, LANES), 0) < lax.broadcasted_iota(jnp.int32, (LANES, LANES), 1)
    ).astype(BF16)

    def norm(src, k, q, h):
        for g in range(half // 16):
            row = h * half + g * 16
            v = src[row : row + 16, :].astype(F32)
            ms = jnp.mean(v * v, axis=-1, keepdims=True)
            hbuf[k, q * LANES + row : q * LANES + row + 16, :] = (v * lax.rsqrt(ms + EPS) * gain).astype(BF16)

    def slots(r):
        first_expert = (me * local_experts).astype(F32)
        eid = lax.broadcasted_iota(jnp.int32, (local_experts, LANES), 0).astype(F32) + first_expert
        rows = []
        for q in range(2):
            ids = ids_all[r, q]
            hit = eid == ids[0:1, :]
            for j in range(1, ids.shape[0]):
                hit = hit | (eid == ids[j : j + 1, :])
            pos = dot(jnp.where(hit, 1.0, 0.0).astype(BF16), tri)
            first = pos < 15.5
            place[r, q] = jnp.where(hit, jnp.where(first, pos, pos + 8.0 * q), -1.0)
            rows.append(jnp.where(hit, jnp.where(first, pos + 16.0 * q, pos + (16.0 + 8.0 * q)), -1.0))
        pair = jnp.concatenate(rows, axis=1)
        slot = lax.broadcasted_iota(jnp.int32, (pair_cap, 2 * LANES), 0).astype(F32)
        for e in range(local_experts):
            oh[r, pl.ds(e * pair_cap, pair_cap), :] = jnp.where(slot == pair[e : e + 1, :], 1.0, 0.0).astype(BF16)

    def gating(r, k):
        logits = lax.dot_general(
            wr_ref[...], hbuf[k], (((1,), (1,)), ((), ())), preferred_element_type=F32
        )
        shifted = jnp.exp(logits - jnp.max(logits, axis=0, keepdims=True))
        prob = shifted / jnp.sum(shifted, axis=0, keepdims=True)
        ids = jnp.concatenate([ids_all[r, 0], ids_all[r, 1]], axis=1)
        eid = lax.broadcasted_iota(jnp.int32, prob.shape, 0).astype(F32)
        chosen = eid == ids[0:1, :]
        for j in range(1, ids.shape[0]):
            chosen = chosen | (eid == ids[j : j + 1, :])
        picked = jnp.where(chosen, prob, 0.0)
        soft[r] = jnp.where(chosen, picked / jnp.sum(picked, axis=0, keepdims=True), 0.0)
        gate = soft[r, pl.ds(pl.multiple_of(me * local_experts, local_experts), local_experts), :]
        slot = lax.broadcasted_iota(jnp.int32, (own_cap, LANES), 0).astype(F32)
        for q in range(2):
            own = place[r, q]
            for e in range(local_experts):
                gates[r, q, pl.ds(e * own_cap, own_cap), :] = jnp.where(
                    slot == own[e : e + 1, :], gate[e : e + 1, q * LANES : (q + 1) * LANES], 0.0
                )

    def gather(r, k):
        for n in range(hidden // COLS):
            cols = slice(n * COLS, (n + 1) * COLS)
            res = dot(oh[r], hbuf[k, :, cols]).astype(BF16)
            for e in range(local_experts):
                xe[e, r * pair_cap : (r + 1) * pair_cap, cols] = res[e * pair_cap : (e + 1) * pair_cap]

    def split_gates(r):
        for q in range(2):
            gt = gates[r, q].T[0:tokens]
            hi = gt.astype(BF16)
            rest = gt - hi.astype(F32)
            mid = rest.astype(BF16)
            low = (rest - mid.astype(F32)).astype(BF16)
            for p, part in enumerate((hi, mid, low)):
                a3[r, q, pl.ds(p * tokens, tokens), :] = part

    own_ids, other_ids = ids_all.at[0, 1], ids_all.at[pl.ds(1, chips - 1)]

    def gate_up_rows(e, rows, after=lambda n: None):
        slot = 2 * (e % (RING // 2))
        data = xe[e, rows, :]
        for n in range(4):
            g = dot(data, wbuf[slot, 2 * n : 2 * n + 2].reshape(hidden, COLS))
            u = dot(data, wbuf[slot + 1, 2 * n : 2 * n + 2].reshape(hidden, COLS))
            act[e, rows, n * COLS : (n + 1) * COLS] = (g * jax.nn.sigmoid(g) * u).astype(BF16)
            after(n)

    own_rows = pl.ds(0, pair_cap)
    rest_rows = pl.ds(pair_cap, (chips - 1) * pair_cap)
    all_rows = pl.ds(0, chips * pair_cap)

    def own_pass(e, carry):
        with jax.named_scope("own_pass"):
            wait_slot(2 * e)
            wait_slot(2 * e + 1)
            gate_up_rows(e, own_rows)
        return carry

    with jax.named_scope("norm_own"):
        norm(x_ref, 0, 0, 0)
        norm(x_ref, 0, 0, 1)
    with jax.named_scope("own_wait"):
        wait_bytes(own_ids, ids_r.at[1])
        c_p.wait_recv()
    with jax.named_scope("prep_own"):
        norm(xbuf.at[0, 1], 0, 1, 0)
        norm(xbuf.at[0, 1], 0, 1, 1)
        slots(0)
        gather(0, 0)
        gating(0, 0)
    lax.fori_loop(0, 1, own_pass, 0)
    with jax.named_scope("slots"):
        wait_bytes(other_ids, ids_r.at[0])
        for r in (last, 1, 2):
            slots(r)
    lax.fori_loop(1, 2, own_pass, 0)
    with jax.named_scope("near_wait"):
        c_r0.wait_recv()
        f_r.start()
        cross[(last, 0)].start()
        c_l1.wait_recv()
        f_l.start()
        cross[(1, 1)].start()
    with jax.named_scope("norm_near"):
        norm(xbuf.at[last, 0], 0, 0, 0)
        norm(xbuf.at[1, 0], 1, 0, 1)
        cross[(last, 0)].wait_recv()
        cross[(1, 1)].wait_recv()
        norm(xbuf.at[last, 1], 0, 1, 0)
        norm(xbuf.at[1, 1], 1, 1, 1)
    lax.fori_loop(2, RING // 2, own_pass, 0)
    with jax.named_scope("near_wait2"):
        c_r1.wait_recv()
        cross[(last, 1)].start()
        c_l0.wait_recv()
        cross[(1, 0)].start()
    with jax.named_scope("norm_near2"):
        norm(xbuf.at[last, 0], 0, 0, 1)
        norm(xbuf.at[1, 0], 1, 0, 0)
        cross[(last, 1)].wait_recv()
        cross[(1, 0)].wait_recv()
        norm(xbuf.at[last, 1], 0, 1, 1)
        norm(xbuf.at[1, 1], 1, 1, 0)
    with jax.named_scope("gather_near"):
        gather(last, 0)
        gather(1, 1)
    with jax.named_scope("far_wait"):
        f_r.wait_recv()
        cross[(2, 0)].start()
        f_l.wait_recv()
        cross[(2, 1)].start()
    with jax.named_scope("gating_near"):
        gating(last, 0)
        gating(1, 1)
    with jax.named_scope("norm_far"):
        norm(xbuf.at[2, 0], 0, 0, 0)
        norm(xbuf.at[2, 0], 0, 0, 1)
    with jax.named_scope("far_cross_wait"):
        wait_bytes(xbuf.at[2, 1], ag_r.at[11])
    with jax.named_scope("norm_far2"):
        norm(xbuf.at[2, 1], 0, 1, 0)
        norm(xbuf.at[2, 1], 0, 1, 1)
    with jax.named_scope("gather_far"):
        gather(2, 0)

    def refill(e):
        def after(n):
            if e < local_experts - RING // 2:
                start_gate_up(e + RING // 2, (n,))
            elif n == 3:
                start_down(e - (local_experts - RING // 2))
        return after

    with jax.named_scope("gate_up_rest"):
        for e in range(RING // 2):
            gate_up_rows(e, rest_rows, refill(e))
            if e == 0:
                gating(2, 0)
            split_gates(far_first[chips - 1 - e])
    for e in range(RING // 2, local_experts):
        slot = 2 * (e % (RING // 2))
        with jax.named_scope("gate_up_wait"):
            wait_slot(slot)
            wait_slot(slot + 1)
        with jax.named_scope("gate_up"):
            gate_up_rows(e, all_rows, refill(e))
    for n in range(RING // 2, chunks):
        start_down(n)

    def cross_copy(n):
        return remote(ps.at[n, 1], d2d.at[n], sum_s.at[0], d2d_r.at[n], peer)

    def far_copies(n):
        return (
            remote(ps.at[n, 0, 2, 0], far.at[n, 0], sum_s.at[1], far_r.at[n], right),
            remote(ps.at[n, 0, 2, 1], far.at[n, 1], sum_s.at[1], far_r.at[n], left),
        )

    def near_copies(n):
        return (
            remote(ps.at[n, 0, 1, 1], fin.at[n, 0, 1], sum_s.at[2], fin_r.at[n], right),
            remote(ps.at[n, 0, last, 0], fin.at[n, 1, 0], sum_s.at[2], fin_r.at[n], left),
        )

    def sum_copies(n):
        return (
            remote(ps.at[n, 0, 1, 0], fin.at[n, 0, 0], sum_s.at[2], fin_r.at[n], right),
            remote(ps.at[n, 0, last, 1], fin.at[n, 1, 1], sum_s.at[2], fin_r.at[n], left),
        )

    def stage1(n):
        with jax.named_scope("cross_wait"):
            cross_copy(n).wait_recv()
        for r in far_first:
            ps[n, 0, r] = ps[n, 0, r] + d2d[n, r]
            if r == 1:
                for c in far_copies(n):
                    c.start()
            if r == last:
                for c in near_copies(n):
                    c.start()

    def chunk(n, carry):
        with jax.named_scope("down_wait"):
            wslot = 2 * lax.rem(n, RING // 2) + n // (RING // 2)
            wait_slot(wslot)
        with jax.named_scope("down"):
            for e in range(local_experts):
                y = dot(act[e], wbuf[wslot, e]).astype(BF16)
                for r in range(chips):
                    base = r * pair_cap
                    both = y[base + 32 : base + 48]
                    for q in range(2):
                        row = e * own_cap
                        ybuf[r, q, row : row + 16, :] = y[base + 16 * q : base + 16 * (q + 1)]
                        ybuf[r, q, row + 16 : row + 32, :] = both

        @pl.when(n > 0)
        def _():
            stage1(n - 1)

        with jax.named_scope("combine"):
            for r in far_first:
                for q in (1, 0):
                    parts = dot(a3[r, q], ybuf[r, q])
                    total = parts[0:tokens] + (parts[tokens : 2 * tokens] + parts[2 * tokens : 3 * tokens])
                    for h in range(2):
                        ps[n, q, r, h] = total[:, h * LANES : (h + 1) * LANES]
        cross_copy(n).start()
        return carry

    lax.fori_loop(0, chunks, chunk, 0)
    wait_bytes(act.at[pl.ds(0, 3)], link_s)
    wait_bytes(xbuf.at[pl.ds(0, 2)], cross_s)
    wait_bytes(own_ids, ids_s.at[1])
    wait_bytes(other_ids, ids_s.at[0])
    stage1(chunks - 1)

    def stage2(n, carry):
        to_right, to_left = sum_copies(n)
        with jax.named_scope("far_sum_wait"):
            wait_bytes(far.at[n], far_r.at[n])
        ps[n, 0, 1, 0] = ps[n, 0, 1, 0] + far[n, 0]
        ps[n, 0, last, 1] = ps[n, 0, last, 1] + far[n, 1]
        to_right.start()
        to_left.start()
        return carry

    with jax.named_scope("stage2"):
        lax.fori_loop(0, chunks, stage2, 0)

    def final(n, carry):
        with jax.named_scope("final_wait"):
            wait_bytes(fin.at[n], fin_r.at[n])
        for h in range(2):
            cols = pl.ds(pl.multiple_of(n * COLS + h * LANES, LANES), LANES)
            total = ps[n, 0, 0, h] + fin[n, 0, h] + fin[n, 1, h]
            out_hbm[:, cols] = (x_ref[:, cols].astype(F32) + total).astype(BF16)
        return carry

    with jax.named_scope("final"):
        lax.fori_loop(0, chunks, final, 0)
    with jax.named_scope("send_wait"):
        wait_bytes(d2d, sum_s.at[0])
        wait_bytes(far, sum_s.at[1])
        wait_bytes(fin, sum_s.at[2])


def solution(mesh):
    group = mesh.shape["ep"]
    chips = group // 2

    def local_block(x_in, norm_gain, w_router, expert_ids, w_gate, w_up, w_down):
        tokens, hidden = x_in.shape
        experts = w_router.shape[1]
        top_k = expert_ids.shape[1]
        local_experts, _, ff = w_gate.shape
        cap = 2 * tokens * top_k // experts
        assert cap == 24 and chips == RING // 2
        chunks = hidden // COLS
        wg = w_gate.reshape(local_experts, 2, hidden // 2, ff)
        wu = w_up.reshape(local_experts, 2, hidden // 2, ff)
        hbm = pl.BlockSpec(memory_space=pl.ANY)
        dma = pltpu.SemaphoreType.DMA
        return pl.pallas_call(
            moe_kernel,
            out_shape=pltpu.VMEM((tokens, hidden), BF16),
            in_specs=[hbm] * 7,
            out_specs=pl.BlockSpec(memory_space=pltpu.VMEM),
            scratch_shapes=[
                pltpu.VMEM((tokens, hidden), BF16),
                pltpu.VMEM((hidden // LANES, LANES), BF16),
                pltpu.VMEM((experts, hidden), BF16),
                pltpu.VMEM((top_k, tokens), jnp.int32),
                pltpu.VMEM((RING, local_experts, ff, COLS), BF16),
                pltpu.VMEM((chips, 2, tokens, hidden), BF16),
                pltpu.VMEM((2, 2 * LANES, hidden), BF16),
                pltpu.VMEM((local_experts, group * cap, hidden), BF16),
                pltpu.VMEM((local_experts, group * cap, ff), BF16),
                pltpu.VMEM((chips, local_experts * 48, 2 * LANES), BF16),
                pltpu.VMEM((chips, 2, local_experts * 32, LANES), F32),
                pltpu.VMEM((chips, 2, 3 * tokens, local_experts * 32), BF16),
                pltpu.VMEM((chips, 2, local_experts * 32, COLS), BF16),
                pltpu.VMEM((chunks, 2, chips, 2, tokens, LANES), F32),
                pltpu.VMEM((chunks, chips, 2, tokens, LANES), F32),
                pltpu.VMEM((chunks, 2, tokens, LANES), F32),
                pltpu.VMEM((chunks, 2, 2, tokens, LANES), F32),
                pltpu.VMEM((chips, 2, top_k, LANES), F32),
                pltpu.VMEM((chips, 2, local_experts, LANES), F32),
                pltpu.VMEM((chips, experts, 2 * LANES), F32),
                dma((4,)), dma((RING,)), dma((2,)), dma((2,)),
                dma, dma, dma((12,)), dma((3,)), dma((chunks,)), dma((chunks,)), dma((chunks,)),
            ],
            compiler_params=pltpu.CompilerParams(
                collective_id=0, has_side_effects=True, vmem_limit_bytes=66600000
            ),
        )(x_in, norm_gain.reshape(hidden // LANES, LANES), w_router.T, expert_ids.T, wg, wu, w_down)

    tok_spec = P(("dp", "ep"), None)
    expert_spec = P("ep", None, None)
    return jax.shard_map(local_block, mesh=mesh, in_specs=(tok_spec, P(None), P(None, None), tok_spec, expert_spec, expert_spec, expert_spec), out_specs=tok_spec, check_vma=False)
```
